1024 devices in a mesh: lon: 256 (over z, y, x_lo), lat: 4 (over x_hi, core).
Axes of the slice: x: 8 (x_hi: 2, x_lo: 4; x = x_hi * 4 + x_lo), y: 8, z: 8, core: 2. Of those that a mesh axis runs over, the one named last changes fastest.
Arguments:
- u_vel: float32 [40, 2048, 2048], P(None, 'lon', 'lat'), may hold values from -6 to 6
- v_vel: float32 [40, 2048, 2048], P(None, 'lon', 'lat'), may hold values from -6 to 6
- thickness: float32 [40], replicated, may hold values from 0.5 to 2
- depth: float32 [2048, 2048], P('lon', 'lat'), may hold values from 0.5 to 2
- sea_mask: int32 [2048, 2048], P('lon', 'lat'), may hold values 0 or 1
- damping: float32 [2048, 2048], P('lon', 'lat'), may hold values from 0.1 to 2
- eta_prev: float32 [2048, 2048], P('lon', 'lat'), may hold values from -6 to 6
Outputs:
- surface: float32 [2048, 2048], P('lon', 'lat')
- residual: float32 [2048, 2048], P('lon', 'lat')
The draws below stay inside these ranges and needn't reach their ends.
All inputs are finite; a program needn't handle non-finite values. No bound on the sum of `sea_mask` on one device may be relied on, other than what follows from the above.
Results may differ from the reference program's by a relative error of at most 0.0003.
Values sent between devices are 32-bit elements; how exact they have to be, the bound alone decides.
No kernel may reach another device: no remote copies, remote signals or barrier semaphores. Data moves between devices by JAX's collectives and lax.ppermute only.
A program may use at most 32 MiB of HBM per device.

```python
import math
import jax
import jax.numpy as jnp
from jax import lax

LEVELS = 40
ITERS = 3
NX = 2048
NY = 2048


def place_ends(values, stream_key, smallest, high):
    longest = values.shape.index(max(values.shape))
    spots = []
    for shift in (0, 1):
        where = [jax.random.randint(jax.random.fold_in(stream_key, axis), (), 0, length) for axis, length in enumerate(values.shape)]
        where[longest] = (where[longest] + shift) % values.shape[longest]
        spots.append(tuple(where))
    return values.at[spots[0]].set(smallest).at[spots[1]].set(high)


def shard_levels(key, shape, split, smallest, high):
    def one(position, parts):
        steps = jax.random.uniform(jax.random.fold_in(jax.random.fold_in(key, 6), position), (parts,), jnp.float32, smallest / len(split), high / len(split))
        return jnp.repeat(jnp.exp(steps), shape[position] // parts).reshape((-1,) + (1,) * (len(shape) - position - 1))

    loudness = one(*split[0])
    for cut in split[1:]:
        loudness = loudness * one(*cut)
    return loudness


def centred(stream_key, dims, scale, reach, split=(), dtype=jnp.bfloat16):
    values = jax.random.normal(stream_key, dims, jnp.float32) * scale
    if len(split) > 0:
        values = shard_levels(stream_key, dims, split, -0.22, 0.18) * values
    return jnp.clip(values, min=-reach, max=reach).astype(dtype)


def setup_inputs(seed: int = 0) -> dict:
    seeds = jax.random.split(jax.random.key(seed), 8)
    return {
        "u_vel": centred(seeds[0], (LEVELS, NX, NY), 1.0, 6.0, ((1, 256), (2, 4)), jnp.float32),
        "v_vel": centred(seeds[1], (LEVELS, NX, NY), 1.0, 6.0, ((1, 256), (2, 4)), jnp.float32),
        "thickness": jnp.clip(jnp.exp(jax.random.uniform(seeds[2], (LEVELS,), jnp.float32, math.log(0.5), math.log(2.0))), 0.5, 2.0),
        "depth": jnp.clip(jnp.exp(math.log(2.0) - 1.3862944 * jax.random.uniform(seeds[3], (NX, NY), jnp.float32) ** shard_levels(seeds[3], (NX, NY), ((0, 256), (1, 4)), -0.2, 0.2)), 0.5, 2.0),
        "sea_mask": place_ends((jax.random.randint(seeds[4], (NX, NY), 0, 8) < 7).astype(jnp.int32), jax.random.fold_in(seeds[4], 1), 0, 1),
        "damping": jnp.clip(jnp.exp(math.log(2.0) - 2.9957323 * jax.random.uniform(seeds[5], (NX, NY), jnp.float32) ** shard_levels(seeds[5], (NX, NY), ((0, 256), (1, 4)), -0.2, 0.2)), 0.1, 2.0),
        "eta_prev": centred(seeds[6], (NX, NY), 1.0, 6.0, ((0, 256), (1, 4)), jnp.float32),
    }


def faces(depth, wet):
    north_ok = (lax.broadcasted_iota(jnp.int32, wet.shape, 1) < wet.shape[1] - 1).astype(jnp.float32)
    wet_east = wet * jnp.roll(wet, -1, 0)
    wet_north = wet * jnp.roll(wet, -1, 1) * north_ok
    face_x = wet_east * 0.5 * (depth + jnp.roll(depth, -1, 0))
    face_y = wet_north * 0.5 * (depth + jnp.roll(depth, -1, 1))
    return (wet_east, wet_north, face_x, face_y)

def operate(field, diag, face_x, face_y):
    result = diag * field - face_x * jnp.roll(field, -1, 0) - jnp.roll(face_x, 1, 0) * jnp.roll(field, 1, 0)
    return result - face_y * jnp.roll(field, -1, 1) - jnp.roll(face_y, 1, 1) * jnp.roll(field, 1, 1)

def reference(u_vel, v_vel, thickness, depth, sea_mask, damping, eta_prev):
    wet = sea_mask.astype(jnp.float32)
    wet_east, wet_north, face_x, face_y = faces(depth, wet)
    scale = 1.0 / math.sqrt(LEVELS)
    east_flux = wet_east * jnp.einsum('k,kxy->xy', thickness, u_vel, precision=lax.Precision.HIGHEST) * scale
    north_flux = wet_north * jnp.einsum('k,kxy->xy', thickness, v_vel, precision=lax.Precision.HIGHEST) * scale
    diverge = east_flux - jnp.roll(east_flux, 1, 0) + north_flux - jnp.roll(north_flux, 1, 1)
    rhs = wet * (damping * eta_prev - diverge)
    diag = damping + face_x + jnp.roll(face_x, 1, 0) + face_y + jnp.roll(face_y, 1, 1)
    surface = jnp.zeros_like(rhs)
    residual = rhs
    precond = residual / diag
    image = operate(precond, diag, face_x, face_y)
    gamma_now = jnp.sum(residual * precond)
    delta_now = jnp.sum(image * precond)
    step_size = gamma_now / delta_now
    direction, along_dir = (precond, image)
    for sweep in range(ITERS):
        surface = surface + step_size * direction
        residual = residual - step_size * along_dir
        if sweep + 1 < ITERS:
            precond = residual / diag
            image = operate(precond, diag, face_x, face_y)
            gamma_next = jnp.sum(residual * precond)
            delta_now = jnp.sum(image * precond)
            ratio_next = gamma_next / gamma_now
            step_size = gamma_next / (delta_now - ratio_next * gamma_next / step_size)
            direction = precond + ratio_next * direction
            along_dir = image + ratio_next * along_dir
            gamma_now = gamma_next
    return (surface, residual)
```

```python
import functools
import math

import jax
import jax.numpy as jnp
from jax import lax
from jax.experimental import pallas as pl
from jax.experimental.pallas import tpu as pltpu
from jax.sharding import Mesh
from jax.sharding import PartitionSpec as P

LEVELS = 40
CHUNKS = 4
ROWS = 8
COLS = 512
FIELDS = 6
LON = ("lon_0", "lon_1", "lon_2")
LAT = ("lat_0", "lat_1")
NEAR = ("lon_2", "lat_0", "lat_1")
FAR = ("lon_0", "lon_1")
SCALE = 1.0 / math.sqrt(LEVELS)
VMEM = pl.BlockSpec(memory_space=pltpu.VMEM)
ANY = pl.BlockSpec(memory_space=pl.ANY)
SMEM = pl.BlockSpec(memory_space=pltpu.SMEM)


def lon_even():
    return lax.rem(lax.axis_index("lon_2"), 2) == 0


def lat_even():
    return lax.axis_index("lat_1") == 0


def pick(flag, yes, no):
    return jnp.where(jnp.full(yes.shape, flag), yes, no)


def sublane(shape):
    return lax.broadcasted_iota(jnp.int32, shape, len(shape) - 2)


def lane(shape):
    return lax.broadcasted_iota(jnp.int32, shape, len(shape) - 1)


def sum_kernel(thick, u, v, depth, mask, damping, eta, own, odd, even, u_buf, v_buf, f_buf, m_buf, sems, f_sems):
    step = LEVELS // CHUNKS
    copies = []
    for c in range(CHUNKS):
        part = pl.ds(c * step, step)
        copies.append(
            (
                pltpu.make_async_copy(u.at[part], u_buf.at[part], sems.at[0, c]),
                pltpu.make_async_copy(v.at[part], v_buf.at[part], sems.at[1, c]),
            )
        )
    small = [
        pltpu.make_async_copy(depth, f_buf.at[0], f_sems.at[0]),
        pltpu.make_async_copy(damping, f_buf.at[1], f_sems.at[1]),
        pltpu.make_async_copy(eta, f_buf.at[2], f_sems.at[2]),
        pltpu.make_async_copy(mask, m_buf, f_sems.at[3]),
    ]
    for a, b in copies:
        a.start()
        b.start()
    for s in small:
        s.start()
    total = [jnp.zeros((ROWS, COLS), jnp.float32), jnp.zeros((ROWS, COLS), jnp.float32)]
    for c in range(CHUNKS):
        for i, buf in enumerate((u_buf, v_buf)):
            copies[c][i].wait()
            for k in range(c * step, (c + 1) * step):
                total[i] = total[i] + thick[k] * buf[k]
    for s in small:
        s.wait()
    wet = m_buf[...].astype(jnp.float32)
    fields = [total[0] * SCALE, total[1] * SCALE, f_buf[0], wet, f_buf[1], f_buf[2]]
    for i, field in enumerate(fields):
        own[i] = field
    high = sublane((ROWS, COLS)) >= ROWS // 2
    flag = lon_even()
    for p in range(FIELDS // 2):
        a, b = fields[2 * p], pltpu.roll(fields[2 * p + 1], ROWS // 2, 0)
        first = jnp.where(high, b, a)
        last = jnp.where(high, a, b)
        even[p] = pick(flag, last, first)
        odd[p] = pick(flag, first, last)


def join_kernel(own, got_odd, got_even, halo, mid, core):
    flag = lon_even()
    side = lat_even()
    high = sublane((ROWS, COLS)) >= ROWS // 2
    rows = []
    for p in range(FIELDS // 2):
        above = pick(flag, got_even[p], got_odd[p])
        below = pick(flag, got_odd[p], got_even[p])
        rows.append(jnp.where(high, below, above))
        rows.append(pltpu.roll(jnp.where(high, above, below), ROWS // 2, 0))
    for i in range(FIELDS):
        halo[i] = rows[i]
        for t, tile in enumerate((own[i], rows[i])):
            first = tile[:, :128]
            last = tile[:, COLS - 128 :]
            core[2 * i + t] = pick(side, last, first)
            mid[2 * i + t] = pick(side, first, last)


def basis_kernel(own, halo, got_mid, got_core, basis, moments):
    side = lat_even()
    right = lane((ROWS, 128)) >= 64
    fields = []
    for i in range(FIELDS):
        tiles = []
        for t, tile in enumerate((own[i], halo[i])):
            above = pick(side, got_core[2 * i + t], got_mid[2 * i + t])
            below = pick(side, got_mid[2 * i + t], got_core[2 * i + t])
            tiles.append(jnp.concatenate([tile, jnp.where(right, below, above)], axis=1))
        fields.append(jnp.concatenate(tiles, axis=0))
    sum_east, sum_north, depth, wet, damping, eta = fields
    rows, cols = 2 * ROWS, COLS + 128

    def east(a):
        return pltpu.roll(a, rows - 1, 0)

    def west(a):
        return pltpu.roll(a, 1, 0)

    def north(a):
        return pltpu.roll(a, cols - 1, 1)

    def south(a):
        return pltpu.roll(a, 1, 1)

    wet_x = wet * east(wet)
    wet_y = wet * north(wet)
    face_x = wet_x * 0.5 * (depth + east(depth))
    face_y = wet_y * 0.5 * (depth + north(depth))
    flux_x = wet_x * sum_east
    flux_y = wet_y * sum_north
    diverge = flux_x - west(flux_x) + flux_y - south(flux_y)
    rhs = wet * (damping * eta - diverge)
    back_x, back_y = west(face_x), south(face_y)
    diag = damping + face_x + back_x + face_y + back_y
    diag = jnp.where(diag > 0.0, diag, 1.0)

    def spread(a):
        return face_x * east(a) + back_x * west(a) + face_y * north(a) + back_y * south(a)

    def mine(a):
        return a[:ROWS, :COLS]

    w0 = rhs
    v0 = w0 / diag
    w1 = spread(v0)
    v1 = w1 / diag
    w2 = spread(v1)
    v2 = w2 / diag
    w3 = spread(v2)
    parts = [mine(a) for a in (v0, v1, v2, w0, w1, w2, w3)]
    for i, part in enumerate(parts):
        basis[i] = part
    v0, v1, v2, w0, w1, w2, w3 = parts
    row = jnp.zeros((1, 128), jnp.float32)
    spot = lane((1, 128))
    for k, (a, b) in enumerate(((v0, w0), (v0, w1), (v1, w1), (v1, w2), (v2, w2), (v2, w3))):
        prod = a * b
        prod = prod[:, :128] + prod[:, 128:256] + (prod[:, 256:384] + prod[:, 384:])
        total = jnp.sum(jnp.sum(prod, axis=0, keepdims=True), axis=1, keepdims=True)
        row = jnp.where(spot == k, total, row)
    moments[...] = jnp.broadcast_to(row, moments.shape)


def relay_kernel(parts, out):
    out[...] = jnp.broadcast_to(jnp.sum(parts[...], axis=0, keepdims=True), out.shape)


def poly(a, b, scale):
    size = max(len(a), len(b))
    out = []
    for i in range(size):
        if i >= len(b):
            out.append(a[i])
        elif i >= len(a):
            out.append(scale * b[i])
        else:
            out.append(a[i] + scale * b[i])
    return out


def dot(a, b, moments, shift=0):
    total = None
    for k in range(len(a) + len(b) - 1):
        coef = None
        for i in range(len(a)):
            j = k - i
            if 0 <= j < len(b):
                term = a[i] * b[j]
                coef = term if coef is None else coef + term
        term = coef * moments[k + shift]
        total = term if total is None else total + term
    return total


def final_kernel(parts, basis, surface, residual):
    row = jnp.sum(parts[...], axis=0, keepdims=True)
    spot = lane((1, 128))
    moments = [jnp.sum(jnp.where(spot == k, row, 0.0), axis=1, keepdims=True) for k in range(6)]
    one = jnp.ones((1, 1), jnp.float32)
    gaps = [moments[k] - moments[k + 1] for k in range(5)]
    pre = [one]
    gamma = moments[0]
    step = gamma / gaps[0]
    direction = pre
    answer = [step]
    for sweep in range(3):
        image = [direction[0]]
        for i in range(1, len(direction)):
            image.append(direction[i] - direction[i - 1])
        image.append(-direction[-1])
        pre = poly(pre, image, -step)
        if sweep == 2:
            break
        gamma_next = dot(pre, pre, moments)
        delta = dot(pre, pre, gaps)
        ratio = gamma_next / gamma
        step = gamma_next / (delta - ratio * gamma_next / step)
        direction = poly(pre, direction, ratio)
        answer = poly(answer, direction, step)
        gamma = gamma_next
    surface[...] = answer[0] * basis[0] + answer[1] * basis[1] + answer[2] * basis[2]
    residual[...] = (pre[0] * basis[3] + pre[1] * basis[4]) + (pre[2] * basis[5] + pre[3] * basis[6])


def shape(*dims):
    return jax.ShapeDtypeStruct(dims, jnp.float32)


def total_over(rows, axes):
    return lax.all_to_all(rows, axes, 0, 0, tiled=True)


def body(u_vel, v_vel, thickness, depth, sea_mask, damping, eta_prev):
    count = lax.axis_size(LON)
    pairs_even = [(i, i ^ 1) for i in range(count)]
    pairs_odd = [(i, (i + 1) % count) if i % 2 else (i, (i - 1) % count) for i in range(count)]
    pairs_core = [(0, 1), (1, 0), (2, 3), (3, 2)]
    pairs_mid = [(1, 2), (2, 1)]
    own, odd, even = pl.pallas_call(
        sum_kernel,
        out_shape=(shape(FIELDS, ROWS, COLS), shape(3, ROWS, COLS), shape(3, ROWS, COLS)),
        in_specs=[SMEM] + [ANY] * 6,
        out_specs=(VMEM, VMEM, VMEM),
        scratch_shapes=[
            pltpu.VMEM((LEVELS, ROWS, COLS), jnp.float32),
            pltpu.VMEM((LEVELS, ROWS, COLS), jnp.float32),
            pltpu.VMEM((3, ROWS, COLS), jnp.float32),
            pltpu.VMEM((ROWS, COLS), jnp.int32),
            pltpu.SemaphoreType.DMA((2, CHUNKS)),
            pltpu.SemaphoreType.DMA((4,)),
        ],
        name="sums",
    )(thickness, u_vel, v_vel, depth, sea_mask, damping, eta_prev)
    got_odd = lax.ppermute(odd, LON, pairs_odd)
    got_even = lax.ppermute(even, LON, pairs_even)
    halo, mid, core = pl.pallas_call(
        join_kernel,
        out_shape=(shape(FIELDS, ROWS, COLS), shape(12, ROWS, 128), shape(12, ROWS, 128)),
        in_specs=[VMEM] * 3,
        out_specs=(VMEM,) * 3,
        name="join",
    )(own, got_odd, got_even)
    got_mid = lax.ppermute(mid, LAT, pairs_mid)
    got_core = lax.ppermute(core, LAT, pairs_core)
    near = lax.axis_size(NEAR)
    far = lax.axis_size(FAR)
    basis, moments = pl.pallas_call(
        basis_kernel,
        out_shape=(shape(7, ROWS, COLS), shape(near, 128)),
        in_specs=[VMEM] * 4,
        out_specs=(VMEM,) * 2,
        name="basis",
    )(own, halo, got_mid, got_core)
    moments = total_over(moments, NEAR)
    moments = pl.pallas_call(
        relay_kernel, out_shape=shape(far, 128), in_specs=[VMEM], out_specs=VMEM, name="relay"
    )(moments)
    moments = total_over(moments, FAR)
    return pl.pallas_call(
        final_kernel,
        out_shape=(shape(ROWS, COLS), shape(ROWS, COLS)),
        in_specs=[VMEM] * 2,
        out_specs=(VMEM,) * 2,
        name="final",
    )(moments, basis)


def solution(mesh):
    torus = Mesh(mesh.devices.reshape(8, 8, 4, 2, 2), LON + LAT)
    wide = P(None, LON, LAT)
    flat = P(LON, LAT)
    return jax.shard_map(
        body,
        mesh=torus,
        in_specs=(wide, wide, P(), flat, flat, flat, flat),
        out_specs=(flat, flat),
        check_vma=False,
    )
```

```python
import functools
import math

import jax
import jax.numpy as jnp
from jax import lax
from jax.experimental import pallas as pl
from jax.experimental.pallas import tpu as pltpu
from jax.sharding import Mesh
from jax.sharding import PartitionSpec as P

LEVELS = 40
CHUNKS = 4
ROWS = 8
COLS = 512
FIELDS = 6
LON = ("lon_0", "lon_1", "lon_2")
LAT = ("lat_0", "lat_1")
NEAR = ("lon_2", "lat_0", "lat_1")
FAR = ("lon_0", "lon_1")
SCALE = 1.0 / math.sqrt(LEVELS)
VMEM = pl.BlockSpec(memory_space=pltpu.VMEM)
ANY = pl.BlockSpec(memory_space=pl.ANY)


def lon_even():
    return lax.rem(lax.axis_index("lon_2"), 2) == 0


def lat_even():
    return lax.axis_index("lat_1") == 0


def pick(flag, yes, no):
    return jnp.where(jnp.full(yes.shape, flag), yes, no)


def turn(tile, lanes):
    return tile if lanes % 128 == 0 else pltpu.roll(tile, lanes % 128, 1)


def sublane(shape):
    return lax.broadcasted_iota(jnp.int32, shape, len(shape) - 2)


def lane(shape):
    return lax.broadcasted_iota(jnp.int32, shape, len(shape) - 1)


def sum_kernel(thick_in, u, v, depth, mask, damping, eta, own, odd, even, u_buf, v_buf, f_buf, m_buf, thick, sems, f_sems):
    step = LEVELS // CHUNKS
    weights = pltpu.make_async_copy(thick_in, thick, f_sems.at[4])
    weights.start()
    copies = []
    for c in range(CHUNKS):
        part = pl.ds(c * step, step)
        copies.append(
            (
                pltpu.make_async_copy(u.at[part], u_buf.at[part], sems.at[0, c]),
                pltpu.make_async_copy(v.at[part], v_buf.at[part], sems.at[1, c]),
            )
        )
    small = [
        pltpu.make_async_copy(depth, f_buf.at[0], f_sems.at[0]),
        pltpu.make_async_copy(damping, f_buf.at[1], f_sems.at[1]),
        pltpu.make_async_copy(eta, f_buf.at[2], f_sems.at[2]),
        pltpu.make_async_copy(mask, m_buf, f_sems.at[3]),
    ]
    for a, b in copies:
        a.start()
        b.start()
    for s in small:
        s.start()
    total = [jnp.zeros((ROWS, COLS), jnp.float32), jnp.zeros((ROWS, COLS), jnp.float32)]
    weights.wait()
    for c in range(CHUNKS):
        for i, buf in enumerate((u_buf, v_buf)):
            copies[c][i].wait()
            for k in range(c * step, (c + 1) * step):
                total[i] = total[i] + thick[k] * buf[k]
    for s in small:
        s.wait()
    wet = m_buf[...].astype(jnp.float32)
    fields = [total[0] * SCALE, total[1] * SCALE, f_buf[0], wet, f_buf[1], f_buf[2]]
    for i, field in enumerate(fields):
        own[i] = field
    high = sublane((ROWS, COLS)) >= ROWS // 2
    flag = lon_even()
    for p in range(FIELDS // 2):
        a, b = fields[2 * p], pltpu.roll(fields[2 * p + 1], ROWS // 2, 0)
        first = jnp.where(high, b, a)
        last = jnp.where(high, a, b)
        even[p] = pick(flag, last, first)
        odd[p] = pick(flag, first, last)


def join_kernel(own, got_odd, got_even, halo, mid, core):
    flag = lon_even()
    side = lat_even()
    high = sublane((ROWS, COLS)) >= ROWS // 2
    rows = []
    for p in range(FIELDS // 2):
        above = pick(flag, got_even[p], got_odd[p])
        below = pick(flag, got_odd[p], got_even[p])
        rows.append(jnp.where(high, below, above))
        rows.append(pltpu.roll(jnp.where(high, above, below), ROWS // 2, 0))
    spot = lane((ROWS, 128))
    first = last = jnp.zeros((ROWS, 128), jnp.float32)
    for i in range(FIELDS):
        halo[i] = rows[i]
        for t, tile in enumerate((own[i], rows[i])):
            at = 8 * (2 * i + t)
            here = jnp.logical_and(spot >= at, spot < at + 4)
            first = jnp.where(here, turn(tile[:, :128], at), first)
            last = jnp.where(here, turn(tile[:, COLS - 128 :], at + 4), last)
    core[...] = pick(side, last, first)
    mid[...] = pick(side, first, last)


def basis_kernel(own, halo, got_mid, got_core, basis, moments):
    side = lat_even()
    right = lane((ROWS, 128)) >= 64
    above = pick(side, got_core[...], got_mid[...])
    below = pick(side, got_mid[...], got_core[...])
    fields = []
    for i in range(FIELDS):
        tiles = []
        for t, tile in enumerate((own[i], halo[i])):
            at = 8 * (2 * i + t)
            edge = jnp.where(right, turn(below, -at - 4), turn(above, -at))
            tiles.append(jnp.concatenate([tile, edge], axis=1))
        fields.append(jnp.concatenate(tiles, axis=0))
    sum_east, sum_north, depth, wet, damping, eta = fields
    rows, cols = 2 * ROWS, COLS + 128

    def east(a):
        return pltpu.roll(a, rows - 1, 0)

    def west(a):
        return pltpu.roll(a, 1, 0)

    def north(a):
        return pltpu.roll(a, cols - 1, 1)

    def south(a):
        return pltpu.roll(a, 1, 1)

    wet_x = wet * east(wet)
    wet_y = wet * north(wet)
    face_x = wet_x * 0.5 * (depth + east(depth))
    face_y = wet_y * 0.5 * (depth + north(depth))
    flux_x = wet_x * sum_east
    flux_y = wet_y * sum_north
    diverge = flux_x - west(flux_x) + flux_y - south(flux_y)
    rhs = wet * (damping * eta - diverge)
    back_x, back_y = west(face_x), south(face_y)
    diag = damping + face_x + back_x + face_y + back_y
    diag = jnp.where(diag > 0.0, diag, 1.0)

    def spread(a):
        return face_x * east(a) + back_x * west(a) + face_y * north(a) + back_y * south(a)

    def mine(a):
        return a[:ROWS, :COLS]

    w0 = rhs
    v0 = w0 / diag
    w1 = spread(v0)
    v1 = w1 / diag
    w2 = spread(v1)
    v2 = w2 / diag
    w3 = spread(v2)
    parts = [mine(a) for a in (v0, v1, v2, w0, w1, w2, w3)]
    for i, part in enumerate(parts):
        basis[i] = part
    v0, v1, v2, w0, w1, w2, w3 = parts
    row = jnp.zeros((1, 128), jnp.float32)
    spot = lane((1, 128))
    for k, (a, b) in enumerate(((v0, w0), (v0, w1), (v1, w1), (v1, w2), (v2, w2), (v2, w3))):
        prod = a * b
        prod = prod[:, :128] + prod[:, 128:256] + (prod[:, 256:384] + prod[:, 384:])
        total = jnp.sum(jnp.sum(prod, axis=0, keepdims=True), axis=1, keepdims=True)
        row = jnp.where(spot == k, total, row)
    moments[...] = jnp.broadcast_to(row, moments.shape)


def relay_kernel(parts, out):
    out[...] = jnp.broadcast_to(jnp.sum(parts[...], axis=0, keepdims=True), out.shape)


def poly(a, b, scale):
    size = max(len(a), len(b))
    out = []
    for i in range(size):
        if i >= len(b):
            out.append(a[i])
        elif i >= len(a):
            out.append(scale * b[i])
        else:
            out.append(a[i] + scale * b[i])
    return out


def dot(a, b, moments, shift=0):
    total = None
    for k in range(len(a) + len(b) - 1):
        coef = None
        for i in range(len(a)):
            j = k - i
            if 0 <= j < len(b):
                term = a[i] * b[j]
                coef = term if coef is None else coef + term
        term = coef * moments[k + shift]
        total = term if total is None else total + term
    return total


def final_kernel(parts, basis, surface, residual):
    row = jnp.sum(parts[...], axis=0, keepdims=True)
    spot = lane((1, 128))
    moments = [jnp.sum(jnp.where(spot == k, row, 0.0), axis=1, keepdims=True) for k in range(6)]
    one = jnp.ones((1, 1), jnp.float32)
    gaps = [moments[k] - moments[k + 1] for k in range(5)]
    pre = [one]
    gamma = moments[0]
    step = gamma / gaps[0]
    direction = pre
    answer = [step]
    for sweep in range(3):
        image = [direction[0]]
        for i in range(1, len(direction)):
            image.append(direction[i] - direction[i - 1])
        image.append(-direction[-1])
        pre = poly(pre, image, -step)
        if sweep == 2:
            break
        gamma_next = dot(pre, pre, moments)
        delta = dot(pre, pre, gaps)
        ratio = gamma_next / gamma
        step = gamma_next / (delta - ratio * gamma_next / step)
        direction = poly(pre, direction, ratio)
        answer = poly(answer, direction, step)
        gamma = gamma_next
    surface[...] = answer[0] * basis[0] + answer[1] * basis[1] + answer[2] * basis[2]
    residual[...] = (pre[0] * basis[3] + pre[1] * basis[4]) + (pre[2] * basis[5] + pre[3] * basis[6])


def kept(*dims):
    return pltpu.VMEM(dims, jnp.float32)


def shape(*dims):
    return jax.ShapeDtypeStruct(dims, jnp.float32)


def call(kernel, name, outs, *args):
    args = [pltpu.with_memory_space_constraint(a, pltpu.VMEM) for a in args]
    specs = jax.tree.map(lambda _: VMEM, outs)
    return pl.pallas_call(kernel, out_shape=outs, in_specs=[VMEM] * len(args), out_specs=specs, name=name)(*args)


def total_over(rows, axes):
    return lax.all_to_all(rows, axes, 0, 0, tiled=True)


def body(u_vel, v_vel, thickness, depth, sea_mask, damping, eta_prev):
    count = lax.axis_size(LON)
    pairs_even = [(i, i ^ 1) for i in range(count)]
    pairs_odd = [(i, (i + 1) % count) if i % 2 else (i, (i - 1) % count) for i in range(count)]
    pairs_core = [(0, 1), (1, 0), (2, 3), (3, 2)]
    pairs_mid = [(1, 2), (2, 1)]
    own, odd, even = pl.pallas_call(
        sum_kernel,
        out_shape=(kept(FIELDS, ROWS, COLS), kept(3, ROWS, COLS), kept(3, ROWS, COLS)),
        in_specs=[ANY] * 7,
        out_specs=(VMEM, VMEM, VMEM),
        scratch_shapes=[
            pltpu.VMEM((LEVELS, ROWS, COLS), jnp.float32),
            pltpu.VMEM((LEVELS, ROWS, COLS), jnp.float32),
            pltpu.VMEM((3, ROWS, COLS), jnp.float32),
            pltpu.VMEM((ROWS, COLS), jnp.int32),
            pltpu.SMEM((LEVELS,), jnp.float32),
            pltpu.SemaphoreType.DMA((2, CHUNKS)),
            pltpu.SemaphoreType.DMA((5,)),
        ],
        name="sums",
    )(thickness, u_vel, v_vel, depth, sea_mask, damping, eta_prev)
    got_odd = lax.ppermute(odd, LON, pairs_odd)
    got_even = lax.ppermute(even, LON, pairs_even)
    outs = (kept(FIELDS, ROWS, COLS), kept(ROWS, 128), kept(ROWS, 128))
    halo, mid, core = call(join_kernel, "join", outs, own, got_odd, got_even)
    got_mid = lax.ppermute(mid, LAT, pairs_mid)
    got_core = lax.ppermute(core, LAT, pairs_core)
    outs = (kept(7, ROWS, COLS), kept(lax.axis_size(NEAR), 128))
    basis, moments = call(basis_kernel, "basis", outs, own, halo, got_mid, got_core)
    moments = total_over(moments, NEAR)
    moments = call(relay_kernel, "relay", kept(lax.axis_size(FAR), 128), moments)
    moments = total_over(moments, FAR)
    return call(final_kernel, "final", (shape(ROWS, COLS), shape(ROWS, COLS)), moments, basis)


def solution(mesh):
    torus = Mesh(mesh.devices.reshape(8, 8, 4, 2, 2), LON + LAT)
    wide = P(None, LON, LAT)
    flat = P(LON, LAT)
    return jax.shard_map(
        body,
        mesh=torus,
        in_specs=(wide, wide, P(), flat, flat, flat, flat),
        out_specs=(flat, flat),
        check_vma=False,
    )
```

```python
import math

import jax
import jax.numpy as jnp
from jax import lax
from jax.experimental import pallas as pl
from jax.experimental.pallas import tpu as pltpu
from jax.sharding import Mesh
from jax.sharding import PartitionSpec as P

LEVELS = 40
CHUNKS = 4
ROWS = 8
COLS = 512
FIELDS = 6
REACH = 4
WIDTH = 7
EDGE = 112
MOMENTS = 122
EDGE_COLS = 256
LON = ("lon_0", "lon_1", "lon_2")
LAT = ("lat_0", "lat_1")
NEAR = ("lon_2", "lat_0", "lat_1")
FAR = ("lon_0", "lon_1")
SCALE = 1.0 / math.sqrt(LEVELS)
VMEM = pl.BlockSpec(memory_space=pltpu.VMEM)
ANY = pl.BlockSpec(memory_space=pl.ANY)


def lon_even():
    return lax.rem(lax.axis_index("lon_2"), 2) == 0


def lat_index():
    return 2 * lax.axis_index("lat_0") + lax.axis_index("lat_1")


def pick(flag, yes, no):
    return jnp.where(jnp.full(yes.shape, flag), yes, no)


def turn(tile, lanes):
    return tile if lanes % 128 == 0 else pltpu.roll(tile, lanes % 128, 1)


def sublane(shape):
    return lax.broadcasted_iota(jnp.int32, shape, len(shape) - 2)


def lane(shape):
    return lax.broadcasted_iota(jnp.int32, shape, len(shape) - 1)


def sum_kernel(thick_in, u, v, depth, mask, damping, eta, own, odd, even, u_buf, v_buf, f_buf, m_buf, thick, sems, f_sems):
    step = LEVELS // CHUNKS
    weights = pltpu.make_async_copy(thick_in, thick, f_sems.at[4])
    weights.start()
    copies = []
    for c in range(CHUNKS):
        part = pl.ds(c * step, step)
        copies.append(
            (
                pltpu.make_async_copy(u.at[part], u_buf.at[part], sems.at[0, c]),
                pltpu.make_async_copy(v.at[part], v_buf.at[part], sems.at[1, c]),
            )
        )
    small = [
        pltpu.make_async_copy(depth, f_buf.at[0], f_sems.at[0]),
        pltpu.make_async_copy(damping, f_buf.at[1], f_sems.at[1]),
        pltpu.make_async_copy(eta, f_buf.at[2], f_sems.at[2]),
        pltpu.make_async_copy(mask, m_buf, f_sems.at[3]),
    ]
    for a, b in copies:
        a.start()
        b.start()
    for s in small:
        s.start()
    total = [jnp.zeros((ROWS, COLS), jnp.float32), jnp.zeros((ROWS, COLS), jnp.float32)]
    weights.wait()
    for c in range(CHUNKS):
        for i, buf in enumerate((u_buf, v_buf)):
            copies[c][i].wait()
            for k in range(c * step, (c + 1) * step):
                total[i] = total[i] + thick[k] * buf[k]
    for s in small:
        s.wait()
    wet = m_buf[...].astype(jnp.float32)
    fields = [total[0] * SCALE, total[1] * SCALE, f_buf[0], wet, f_buf[1], f_buf[2]]
    for i, field in enumerate(fields):
        own[i] = field
    high = sublane((ROWS, COLS)) >= ROWS // 2
    flag = lon_even()
    for p in range(FIELDS // 2):
        a, b = fields[2 * p], pltpu.roll(fields[2 * p + 1], ROWS // 2, 0)
        first = jnp.where(high, b, a)
        last = jnp.where(high, a, b)
        even[p] = pick(flag, last, first)
        odd[p] = pick(flag, first, last)


def stencil(face_x, face_y, rhs, diag):
    rows, cols = rhs.shape
    back_x, back_y = pltpu.roll(face_x, 1, 0), pltpu.roll(face_y, 1, 1)
    diag = jnp.where(diag > 0.0, diag, 1.0)

    def spread(a):
        ends = face_x * pltpu.roll(a, rows - 1, 0) + back_x * pltpu.roll(a, 1, 0)
        return ends + face_y * pltpu.roll(a, cols - 1, 1) + back_y * pltpu.roll(a, 1, 1)

    w0 = rhs
    v0 = w0 / diag
    w1 = spread(v0)
    v1 = w1 / diag
    w2 = spread(v1)
    v2 = w2 / diag
    w3 = spread(v2)
    return [a[:ROWS] for a in (v0, v1, v2, w0, w1, w2, w3)]


def add_moments(basis, keep, first):
    v0, v1, v2, w0, w1, w2, w3 = basis
    row = jnp.zeros((1, 128), jnp.float32)
    spot = lane((1, 128))
    for k, (a, b) in enumerate(((v0, w0), (v0, w1), (v1, w1), (v1, w2), (v2, w2), (v2, w3))):
        prod = jnp.where(keep, a * b, 0.0)
        tiles = [prod[:, i : i + 128] for i in range(0, prod.shape[1], 128)]
        while len(tiles) > 1:
            tiles = [tiles[i] + tiles[i + 1] for i in range(0, len(tiles), 2)]
        total = jnp.sum(jnp.sum(tiles[0], axis=0, keepdims=True), axis=1, keepdims=True)
        row = jnp.where(spot == first + k, total, row)
    return row


def block_kernel(own, got_odd, got_even, basis, slots):
    flag = lon_even()
    high = sublane((ROWS, COLS)) >= ROWS // 2
    rows = []
    for p in range(FIELDS // 2):
        above = pick(flag, got_even[p], got_odd[p])
        below = pick(flag, got_odd[p], got_even[p])
        rows.append(jnp.where(high, below, above))
        rows.append(pltpu.roll(jnp.where(high, above, below), ROWS // 2, 0))
    fields = [jnp.concatenate([own[i], rows[i]], axis=0) for i in range(FIELDS)]
    sum_east, sum_north, depth, wet, damping, eta = fields
    inner = lane(wet.shape) < COLS - 1
    wet_x = wet * pltpu.roll(wet, 2 * ROWS - 1, 0)
    wet_y = jnp.where(inner, wet * pltpu.roll(wet, COLS - 1, 1), 0.0)
    face_x = wet_x * 0.5 * (depth + pltpu.roll(depth, 2 * ROWS - 1, 0))
    face_y = wet_y * 0.5 * (depth + pltpu.roll(depth, COLS - 1, 1))
    flux_x = wet_x * sum_east
    flux_y = wet_y * sum_north
    diverge = flux_x - pltpu.roll(flux_x, 1, 0) + flux_y - pltpu.roll(flux_y, 1, 1)
    rhs = wet * (damping * eta - diverge)
    diag = damping + face_x + pltpu.roll(face_x, 1, 0) + face_y + pltpu.roll(face_y, 1, 1)
    parts = stencil(face_x, face_y, rhs, diag)
    for i, part in enumerate(parts):
        basis[i] = part
    place = lat_index()
    spot = lane((ROWS, COLS))
    low = jnp.where(place == 0, 0, REACH)
    top = jnp.where(place == lax.axis_size(LAT) - 1, COLS, COLS - REACH)
    keep = jnp.logical_and(spot >= low, spot < top)
    row = add_moments(parts, keep, MOMENTS)
    spot = lane((ROWS, 128))
    tile = jnp.where(sublane((ROWS, 128)) == 0, row, 0.0)
    pieces = []
    for t in range(2):
        for i, field in enumerate((rhs, diag, face_x, face_y)):
            at = 2 * WIDTH * (4 * t + i)
            pieces.append((field, t, COLS - WIDTH, at, WIDTH))
            pieces.append((field, t, 0, at + WIDTH, WIDTH))
        for i, field in enumerate((wet, depth, sum_north)):
            pieces.append((field, t, COLS - 1, EDGE + 2 * i + t, 1))
        for i, field in enumerate((wet, depth)):
            pieces.append((field, t, 0, EDGE + 6 + 2 * i + t, 1))
    for field, t, start, at, size in pieces:
        base = start - start % 128
        moved = turn(field[ROWS * t : ROWS * (t + 1), base : base + 128], at - start % 128)
        tile = jnp.where(jnp.logical_and(spot >= at, spot < at + size), moved, tile)
    for i in range(slots.shape[0]):
        slots[i] = tile


def edge_kernel(slots, edge_basis, moments):
    spot = lane((ROWS, 128))
    count = lax.axis_size(LAT)
    group = slots.shape[0]
    left = jnp.logical_and(spot < EDGE, lax.rem(spot, 2 * WIDTH) < WIDTH)
    left = jnp.logical_or(left, jnp.logical_and(spot >= EDGE, spot < EDGE + 6))
    tiles = EDGE_COLS // 128
    zero = jnp.zeros((ROWS, 128), jnp.float32)
    fields = [[[zero for _ in range(tiles)] for _ in range(2)] for _ in range(6)]
    for b in range(group // count * (count - 1)):
        slot = b // (count - 1) * count + b % (count - 1)
        pair = jnp.where(left, slots[slot], slots[slot + 1])
        far = turn(pair, -6)
        wets = pair * far
        face = wets * 0.5 * turn(pair + far, -2)
        flux = wets * turn(pair, -4)
        at, home = 16 * (b % 8), b // 8
        here = jnp.logical_and(spot >= at, spot < at + 2 * WIDTH)
        seam = spot == at + WIDTH - 1
        for t in range(2):
            for i in range(4):
                moved = turn(pair, at - 2 * WIDTH * (4 * t + i))
                fields[i][t][home] = jnp.where(here, moved, fields[i][t][home])
            for i, value in enumerate((face, flux)):
                moved = turn(value, at + WIDTH - 1 - EDGE - t)
                fields[4 + i][t][home] = jnp.where(seam, moved, fields[4 + i][t][home])
    fields = [jnp.concatenate([jnp.concatenate(f[t], axis=1) for t in range(2)], axis=0) for f in fields]
    rhs, diag, face_x, face_y, face, flux = fields
    rhs = rhs - flux + pltpu.roll(flux, 1, 1)
    diag = diag + face + pltpu.roll(face, 1, 1)
    face_y = face_y + face
    parts = stencil(face_x, face_y, rhs, diag)
    for i, part in enumerate(parts):
        edge_basis[i] = part
    spot = lane((ROWS, EDGE_COLS))
    column = lax.rem(spot, 16)
    keep = jnp.logical_and(column >= WIDTH - REACH, column < WIDTH + REACH)
    row = add_moments(parts, keep, MOMENTS)
    total = slots[0]
    for i in range(1, group):
        total = total + slots[i]
    total = total[:1] + row
    moments[...] = jnp.broadcast_to(total, moments.shape)


def poly(a, b, scale):
    size = max(len(a), len(b))
    out = []
    for i in range(size):
        if i >= len(b):
            out.append(a[i])
        elif i >= len(a):
            out.append(scale * b[i])
        else:
            out.append(a[i] + scale * b[i])
    return out


def dot(a, b, moments, shift=0):
    total = None
    for k in range(len(a) + len(b) - 1):
        coef = None
        for i in range(len(a)):
            j = k - i
            if 0 <= j < len(b):
                term = a[i] * b[j]
                coef = term if coef is None else coef + term
        term = coef * moments[k + shift]
        total = term if total is None else total + term
    return total


def final_kernel(parts, basis, edge_basis, surface, residual):
    row = jnp.sum(parts[...], axis=0, keepdims=True)
    spot = lane((1, 128))
    moments = [jnp.sum(jnp.where(spot == MOMENTS + k, row, 0.0), axis=1, keepdims=True) for k in range(6)]
    one = jnp.ones((1, 1), jnp.float32)
    gaps = [moments[k] - moments[k + 1] for k in range(5)]
    pre = [one]
    gamma = moments[0]
    step = gamma / gaps[0]
    direction = pre
    answer = [step]
    for sweep in range(3):
        image = [direction[0]]
        for i in range(1, len(direction)):
            image.append(direction[i] - direction[i - 1])
        image.append(-direction[-1])
        pre = poly(pre, image, -step)
        if sweep == 2:
            break
        gamma_next = dot(pre, pre, moments)
        delta = dot(pre, pre, gaps)
        ratio = gamma_next / gamma
        step = gamma_next / (delta - ratio * gamma_next / step)
        direction = poly(pre, direction, ratio)
        answer = poly(answer, direction, step)
        gamma = gamma_next

    def combine(b):
        eta = answer[0] * b[0] + answer[1] * b[1] + answer[2] * b[2]
        return eta, (pre[0] * b[3] + pre[1] * b[4]) + (pre[2] * b[5] + pre[3] * b[6])

    inner, edge = combine(basis), combine(edge_basis)
    place, count = lat_index(), lax.axis_size(LAT)
    group = lax.axis_index("lon_2") * (count - 1)
    spot = lane((ROWS, 128))
    for out, body, strip in ((surface, inner[0], edge[0]), (residual, inner[1], edge[1])):
        out[:, 128 : COLS - 128] = body[:, 128 : COLS - 128]
        for side, ok, base, near in ((-1, place > 0, 0, spot < REACH), (0, place < count - 1, COLS - 128, spot >= 128 - REACH)):
            b = group + place + side
            tile = strip[:, :128]
            for i in range(1, EDGE_COLS // 128):
                tile = pick(b // 8 == i, strip[:, 128 * i : 128 * (i + 1)], tile)
            start = 16 * lax.rem(b, 8) + WIDTH
            moved = pltpu.roll(tile, lax.rem(256 - start, 128), 1)
            use = jnp.logical_and(near, ok)
            out[:, base : base + 128] = jnp.where(use, moved, body[:, base : base + 128])


def kept(*dims):
    return pltpu.VMEM(dims, jnp.float32)


def shape(*dims):
    return jax.ShapeDtypeStruct(dims, jnp.float32)


def call(kernel, name, outs, *args):
    args = [pltpu.with_memory_space_constraint(a, pltpu.VMEM) for a in args]
    specs = jax.tree.map(lambda _: VMEM, outs)
    return pl.pallas_call(kernel, out_shape=outs, in_specs=[VMEM] * len(args), out_specs=specs, name=name)(*args)


def body(u_vel, v_vel, thickness, depth, sea_mask, damping, eta_prev):
    count = lax.axis_size(LON)
    pairs_even = [(i, i ^ 1) for i in range(count)]
    pairs_odd = [(i, (i + 1) % count) if i % 2 else (i, (i - 1) % count) for i in range(count)]
    own, odd, even = pl.pallas_call(
        sum_kernel,
        out_shape=(kept(FIELDS, ROWS, COLS), kept(3, ROWS, COLS), kept(3, ROWS, COLS)),
        in_specs=[ANY] * 7,
        out_specs=(VMEM, VMEM, VMEM),
        scratch_shapes=[
            pltpu.VMEM((LEVELS, ROWS, COLS), jnp.float32),
            pltpu.VMEM((LEVELS, ROWS, COLS), jnp.float32),
            pltpu.VMEM((3, ROWS, COLS), jnp.float32),
            pltpu.VMEM((ROWS, COLS), jnp.int32),
            pltpu.SMEM((LEVELS,), jnp.float32),
            pltpu.SemaphoreType.DMA((2, CHUNKS)),
            pltpu.SemaphoreType.DMA((5,)),
        ],
        name="sums",
    )(thickness, u_vel, v_vel, depth, sea_mask, damping, eta_prev)
    got_odd = lax.ppermute(odd, LON, pairs_odd)
    got_even = lax.ppermute(even, LON, pairs_even)
    near, far = lax.axis_size(NEAR), lax.axis_size(FAR)
    basis, slots = call(block_kernel, "block", (kept(7, ROWS, COLS), kept(near, ROWS, 128)), own, got_odd, got_even)
    slots = lax.all_to_all(slots, NEAR, 0, 0, tiled=True)
    edge_basis, moments = call(edge_kernel, "edge", (kept(7, ROWS, EDGE_COLS), kept(far, 128)), slots)
    moments = lax.all_to_all(moments, FAR, 0, 0, tiled=True)
    outs = (shape(ROWS, COLS), shape(ROWS, COLS))
    return call(final_kernel, "final", outs, moments, basis, edge_basis)


def solution(mesh):
    torus = Mesh(mesh.devices.reshape(8, 8, 4, 2, 2), LON + LAT)
    wide = P(None, LON, LAT)
    flat = P(LON, LAT)
    return jax.shard_map(
        body,
        mesh=torus,
        in_specs=(wide, wide, P(), flat, flat, flat, flat),
        out_specs=(flat, flat),
        check_vma=False,
    )
```

```python
import math

import jax
import jax.numpy as jnp
from jax import lax
from jax.experimental import pallas as pl
from jax.experimental.pallas import tpu as pltpu
from jax.sharding import Mesh
from jax.sharding import PartitionSpec as P

LEVELS = 40
CHUNKS = 4
ROWS = 8
COLS = 512
FIELDS = 6
REACH = 4
WIDTH = 7
EDGE = 112
MOMENTS = 122
PLAIN = 116
EDGE_COLS = 256
LON = ("lon_0", "lon_1", "lon_2")
LAT = ("lat_0", "lat_1")
NEAR = ("lon_2", "lat_0", "lat_1")
FAR = ("lon_0", "lon_1")
SCALE = 1.0 / math.sqrt(LEVELS)
VMEM = pl.BlockSpec(memory_space=pltpu.VMEM)
ANY = pl.BlockSpec(memory_space=pl.ANY)


def lon_even():
    return lax.rem(lax.axis_index("lon_2"), 2) == 0


def lat_index():
    return 2 * lax.axis_index("lat_0") + lax.axis_index("lat_1")


def pick(flag, yes, no):
    return jnp.where(jnp.full(yes.shape, flag), yes, no)


def turn(tile, lanes):
    return tile if lanes % 128 == 0 else pltpu.roll(tile, lanes % 128, 1)


def sublane(shape):
    return lax.broadcasted_iota(jnp.int32, shape, len(shape) - 2)


def lane(shape):
    return lax.broadcasted_iota(jnp.int32, shape, len(shape) - 1)


def sum_kernel(thick_in, u, v, depth, mask, damping, eta, own, odd, even, u_buf, v_buf, f_buf, m_buf, thick, sems, f_sems):
    step = LEVELS // CHUNKS
    weights = pltpu.make_async_copy(thick_in, thick, f_sems.at[4])
    weights.start()
    copies = []
    for c in range(CHUNKS):
        part = pl.ds(c * step, step)
        copies.append(
            (
                pltpu.make_async_copy(u.at[part], u_buf.at[part], sems.at[0, c]),
                pltpu.make_async_copy(v.at[part], v_buf.at[part], sems.at[1, c]),
            )
        )
    small = [
        pltpu.make_async_copy(depth, f_buf.at[0], f_sems.at[0]),
        pltpu.make_async_copy(damping, f_buf.at[1], f_sems.at[1]),
        pltpu.make_async_copy(eta, f_buf.at[2], f_sems.at[2]),
        pltpu.make_async_copy(mask, m_buf, f_sems.at[3]),
    ]
    for a, b in copies:
        a.start()
        b.start()
    for s in small:
        s.start()
    total = [jnp.zeros((ROWS, COLS), jnp.float32), jnp.zeros((ROWS, COLS), jnp.float32)]
    weights.wait()
    for c in range(CHUNKS):
        for i, buf in enumerate((u_buf, v_buf)):
            copies[c][i].wait()
            for k in range(c * step, (c + 1) * step):
                total[i] = total[i] + thick[k] * buf[k]
    for s in small:
        s.wait()
    wet = m_buf[...].astype(jnp.float32)
    fields = [total[0] * SCALE, total[1] * SCALE, f_buf[0], wet, f_buf[1], f_buf[2]]
    for i, field in enumerate(fields):
        own[i] = field
    high = sublane((ROWS, COLS)) >= ROWS // 2
    flag = lon_even()
    for p in range(FIELDS // 2):
        a, b = fields[2 * p], pltpu.roll(fields[2 * p + 1], ROWS // 2, 0)
        first = jnp.where(high, b, a)
        last = jnp.where(high, a, b)
        even[p] = pick(flag, last, first)
        odd[p] = pick(flag, first, last)


def stencil(face_x, face_y, rhs, diag):
    rows, cols = rhs.shape
    back_x, back_y = pltpu.roll(face_x, 1, 0), pltpu.roll(face_y, 1, 1)
    diag = jnp.where(diag > 0.0, diag, 1.0)

    def spread(a):
        ends = face_x * pltpu.roll(a, rows - 1, 0) + back_x * pltpu.roll(a, 1, 0)
        return ends + face_y * pltpu.roll(a, cols - 1, 1) + back_y * pltpu.roll(a, 1, 1)

    w0 = rhs
    v0 = w0 / diag
    w1 = diag * v0 - spread(v0)
    v1 = w1 / diag
    w2 = -spread(v1)
    v2 = w2 / diag
    w3 = -spread(v2)
    return [a[:ROWS] for a in (v0, v1, v2, w0, w1, w2, w3)]


def add_moments(basis, keep):
    s0, s1, s2, w0, w1, w2, w3 = basis
    n1, n2 = s0 - s1, s0 - s1 + s2
    m1 = w0 - w1
    m2 = m1 + w2
    m3 = m2 - w3
    plain = ((s0, m1), (n1, m1), (n1, m2), (n2, m2), (n2, m3))
    newton = ((s0, w0), (s0, w1), (s1, w1), (s1, w2), (s2, w2), (s2, w3))
    row = jnp.zeros((1, 128), jnp.float32)
    spot = lane((1, 128))
    for at, (a, b) in (*enumerate(plain, PLAIN), *enumerate(newton, MOMENTS)):
        prod = jnp.where(keep, a * b, 0.0)
        tiles = [prod[:, i : i + 128] for i in range(0, prod.shape[1], 128)]
        while len(tiles) > 1:
            tiles = [tiles[i] + tiles[i + 1] for i in range(0, len(tiles), 2)]
        total = jnp.sum(jnp.sum(tiles[0], axis=0, keepdims=True), axis=1, keepdims=True)
        row = jnp.where(spot == at, total, row)
    return row


def block_kernel(own, got_odd, got_even, basis, slots):
    flag = lon_even()
    high = sublane((ROWS, COLS)) >= ROWS // 2
    rows = []
    for p in range(FIELDS // 2):
        above = pick(flag, got_even[p], got_odd[p])
        below = pick(flag, got_odd[p], got_even[p])
        rows.append(jnp.where(high, below, above))
        rows.append(pltpu.roll(jnp.where(high, above, below), ROWS // 2, 0))
    fields = [jnp.concatenate([own[i], rows[i]], axis=0) for i in range(FIELDS)]
    sum_east, sum_north, depth, wet, damping, eta = fields
    inner = lane(wet.shape) < COLS - 1
    wet_x = wet * pltpu.roll(wet, 2 * ROWS - 1, 0)
    wet_y = jnp.where(inner, wet * pltpu.roll(wet, COLS - 1, 1), 0.0)
    face_x = wet_x * 0.5 * (depth + pltpu.roll(depth, 2 * ROWS - 1, 0))
    face_y = wet_y * 0.5 * (depth + pltpu.roll(depth, COLS - 1, 1))
    flux_x = wet_x * sum_east
    flux_y = wet_y * sum_north
    diverge = flux_x - pltpu.roll(flux_x, 1, 0) + flux_y - pltpu.roll(flux_y, 1, 1)
    rhs = wet * (damping * eta - diverge)
    diag = damping + face_x + pltpu.roll(face_x, 1, 0) + face_y + pltpu.roll(face_y, 1, 1)
    parts = stencil(face_x, face_y, rhs, diag)
    for i, part in enumerate(parts):
        basis[i] = part
    place = lat_index()
    spot = lane((ROWS, COLS))
    low = jnp.where(place == 0, 0, REACH)
    top = jnp.where(place == lax.axis_size(LAT) - 1, COLS, COLS - REACH)
    keep = jnp.logical_and(spot >= low, spot < top)
    row = jnp.broadcast_to(add_moments(parts, keep), (ROWS, 128))
    spot = lane((ROWS, 128))
    deep = sublane((ROWS, 128))
    tile = jnp.where(deep == 0, row, jnp.where(deep == 1, turn(row, MOMENTS - PLAIN), 0.0))
    pieces = []
    for t in range(2):
        for i, field in enumerate((rhs, diag, face_x, face_y)):
            at = 2 * WIDTH * (4 * t + i)
            pieces.append((field, t, COLS - WIDTH, at, WIDTH))
            pieces.append((field, t, 0, at + WIDTH, WIDTH))
        for i, field in enumerate((wet, depth, sum_north)):
            pieces.append((field, t, COLS - 1, EDGE + 2 * i + t, 1))
        for i, field in enumerate((wet, depth)):
            pieces.append((field, t, 0, EDGE + 6 + 2 * i + t, 1))
    for field, t, start, at, size in pieces:
        base = start - start % 128
        moved = turn(field[ROWS * t : ROWS * (t + 1), base : base + 128], at - start % 128)
        tile = jnp.where(jnp.logical_and(spot >= at, spot < at + size), moved, tile)
    for i in range(slots.shape[0]):
        slots[i] = tile


def edge_kernel(slots, edge_basis, moments):
    spot = lane((ROWS, 128))
    count = lax.axis_size(LAT)
    group = slots.shape[0]
    left = jnp.logical_and(spot < EDGE, lax.rem(spot, 2 * WIDTH) < WIDTH)
    left = jnp.logical_or(left, jnp.logical_and(spot >= EDGE, spot < EDGE + 6))
    tiles = EDGE_COLS // 128
    zero = jnp.zeros((ROWS, 128), jnp.float32)
    fields = [[[zero for _ in range(tiles)] for _ in range(2)] for _ in range(6)]
    for b in range(group // count * (count - 1)):
        slot = b // (count - 1) * count + b % (count - 1)
        pair = jnp.where(left, slots[slot], slots[slot + 1])
        far = turn(pair, -6)
        wets = pair * far
        face = wets * 0.5 * turn(pair + far, -2)
        flux = wets * turn(pair, -4)
        at, home = 16 * (b % 8), b // 8
        here = jnp.logical_and(spot >= at, spot < at + 2 * WIDTH)
        seam = spot == at + WIDTH - 1
        for t in range(2):
            for i in range(4):
                moved = turn(pair, at - 2 * WIDTH * (4 * t + i))
                fields[i][t][home] = jnp.where(here, moved, fields[i][t][home])
            for i, value in enumerate((face, flux)):
                moved = turn(value, at + WIDTH - 1 - EDGE - t)
                fields[4 + i][t][home] = jnp.where(seam, moved, fields[4 + i][t][home])
    fields = [jnp.concatenate([jnp.concatenate(f[t], axis=1) for t in range(2)], axis=0) for f in fields]
    rhs, diag, face_x, face_y, face, flux = fields
    rhs = rhs - flux + pltpu.roll(flux, 1, 1)
    diag = diag + face + pltpu.roll(face, 1, 1)
    face_y = face_y + face
    parts = stencil(face_x, face_y, rhs, diag)
    for i, part in enumerate(parts):
        edge_basis[i] = part
    spot = lane((ROWS, EDGE_COLS))
    column = lax.rem(spot, 16)
    keep = jnp.logical_and(column >= WIDTH - REACH, column < WIDTH + REACH)
    row = add_moments(parts, keep)
    sums = [slots[i] for i in range(group)]
    while len(sums) > 1:
        sums = [sums[i] + sums[i + 1] for i in range(0, len(sums), 2)]
    total = jnp.where(lane((ROWS, 128)) >= MOMENTS, sums[0], pltpu.roll(turn(sums[0], PLAIN - MOMENTS), ROWS - 1, 0))
    moments[...] = jnp.broadcast_to(total[:1] + row, moments.shape)


def poly(a, b, scale):
    size = max(len(a), len(b))
    out = []
    for i in range(size):
        if i >= len(b):
            out.append(a[i])
        elif i >= len(a):
            out.append(scale * b[i])
        else:
            out.append(a[i] + scale * b[i])
    return out


def square(a, gram):
    total = None
    for i in range(len(a)):
        for j in range(i, len(a)):
            term = a[i] * a[j] * gram[i, j]
            term = term if i == j else 2.0 * term
            total = term if total is None else total + term
    return total


def final_kernel(parts, basis, edge_basis, surface, residual):
    row = jnp.sum(parts[...], axis=0, keepdims=True)
    spot = lane((1, 128))
    def at(k):
        return jnp.sum(jnp.where(spot == k, row, 0.0), axis=1, keepdims=True)

    g00, g01, g11, g12, g22, g23 = [at(MOMENTS + k) for k in range(6)]
    m1, m2, m3, m4, m5 = [at(PLAIN + k) for k in range(5)]
    rough = g01 > 0.5 * g00
    newton = {(0, 0): g00, (0, 1): g01, (1, 1): g11, (0, 2): g11 - g01, (1, 2): g12, (2, 2): g22}
    plain = {(0, 0): g00, (0, 1): m1, (1, 1): m2, (0, 2): m2, (1, 2): m3, (2, 2): m4}
    gram = {k: jnp.where(rough, plain[k], newton[k]) for k in plain}
    newton = {(0, 0): g01, (0, 1): g11, (1, 1): g12 + g11, (0, 2): g12, (1, 2): g22 + g12, (2, 2): g23 + g22}
    plain = {(0, 0): g00 - m1, (0, 1): m1 - m2, (1, 1): m2 - m3, (0, 2): m2 - m3, (1, 2): m3 - m4, (2, 2): m4 - m5}
    energy = {k: jnp.where(rough, plain[k], newton[k]) for k in plain}
    stay, shift = jnp.where(rough, 1.0, 0.0), jnp.where(rough, -1.0, 1.0)
    one = jnp.ones((1, 1), jnp.float32)
    pre, direction = [one], [one]
    gamma = g00
    step = gamma / energy[0, 0]
    answer = [step]
    for sweep in range(3):
        image = [stay * direction[0]]
        for i in range(1, sweep + 1):
            image.append(direction[i] + shift * direction[i - 1])
        image.append(shift * direction[-1])
        pre = poly(pre, image, -step)
        if sweep == 2:
            break
        gamma_next = square(pre, gram)
        delta = square(pre, energy)
        ratio = gamma_next / gamma
        step = gamma_next / (delta - ratio * gamma_next / step)
        direction = poly(pre, direction, ratio)
        answer = poly(answer, direction, step)
        gamma = gamma_next
    for coefs in (answer, pre):
        for i in range(len(coefs) - 1, 0, -1):
            coefs[i - 1] = coefs[i - 1] + jnp.where(rough, coefs[i], 0.0)
        for i in range(1, len(coefs), 2):
            coefs[i] = shift * coefs[i]

    def combine(b):
        eta = answer[0] * b[0] + answer[1] * b[1] + answer[2] * b[2]
        return eta, (pre[0] * b[3] + pre[1] * b[4]) + (pre[2] * b[5] + pre[3] * b[6])

    inner, edge = combine(basis), combine(edge_basis)
    place, count = lat_index(), lax.axis_size(LAT)
    group = lax.axis_index("lon_2") * (count - 1)
    spot = lane((ROWS, 128))
    for out, body, strip in ((surface, inner[0], edge[0]), (residual, inner[1], edge[1])):
        out[:, 128 : COLS - 128] = body[:, 128 : COLS - 128]
        for side, ok, base, near in ((-1, place > 0, 0, spot < REACH), (0, place < count - 1, COLS - 128, spot >= 128 - REACH)):
            b = group + place + side
            tile = strip[:, :128]
            for i in range(1, EDGE_COLS // 128):
                tile = pick(b // 8 == i, strip[:, 128 * i : 128 * (i + 1)], tile)
            start = 16 * lax.rem(b, 8) + WIDTH
            moved = pltpu.roll(tile, lax.rem(256 - start, 128), 1)
            use = jnp.logical_and(near, ok)
            out[:, base : base + 128] = jnp.where(use, moved, body[:, base : base + 128])


def kept(*dims):
    return pltpu.VMEM(dims, jnp.float32)


def shape(*dims):
    return jax.ShapeDtypeStruct(dims, jnp.float32)


def call(kernel, name, outs, *args):
    args = [pltpu.with_memory_space_constraint(a, pltpu.VMEM) for a in args]
    specs = jax.tree.map(lambda _: VMEM, outs)
    return pl.pallas_call(kernel, out_shape=outs, in_specs=[VMEM] * len(args), out_specs=specs, name=name)(*args)


def body(u_vel, v_vel, thickness, depth, sea_mask, damping, eta_prev):
    count = lax.axis_size(LON)
    pairs_even = [(i, i ^ 1) for i in range(count)]
    pairs_odd = [(i, (i + 1) % count) if i % 2 else (i, (i - 1) % count) for i in range(count)]
    own, odd, even = pl.pallas_call(
        sum_kernel,
        out_shape=(kept(FIELDS, ROWS, COLS), kept(3, ROWS, COLS), kept(3, ROWS, COLS)),
        in_specs=[ANY] * 7,
        out_specs=(VMEM, VMEM, VMEM),
        scratch_shapes=[
            pltpu.VMEM((LEVELS, ROWS, COLS), jnp.float32),
            pltpu.VMEM((LEVELS, ROWS, COLS), jnp.float32),
            pltpu.VMEM((3, ROWS, COLS), jnp.float32),
            pltpu.VMEM((ROWS, COLS), jnp.int32),
            pltpu.SMEM((LEVELS,), jnp.float32),
            pltpu.SemaphoreType.DMA((2, CHUNKS)),
            pltpu.SemaphoreType.DMA((5,)),
        ],
        name="sums",
    )(thickness, u_vel, v_vel, depth, sea_mask, damping, eta_prev)
    got_odd = lax.ppermute(odd, LON, pairs_odd)
    got_even = lax.ppermute(even, LON, pairs_even)
    near, far = lax.axis_size(NEAR), lax.axis_size(FAR)
    basis, slots = call(block_kernel, "block", (kept(7, ROWS, COLS), kept(near, ROWS, 128)), own, got_odd, got_even)
    slots = lax.all_to_all(slots, NEAR, 0, 0, tiled=True)
    edge_basis, moments = call(edge_kernel, "edge", (kept(7, ROWS, EDGE_COLS), kept(far, 128)), slots)
    moments = lax.all_to_all(moments, FAR, 0, 0, tiled=True)
    outs = (shape(ROWS, COLS), shape(ROWS, COLS))
    return call(final_kernel, "final", outs, moments, basis, edge_basis)


def solution(mesh):
    torus = Mesh(mesh.devices.reshape(8, 8, 4, 2, 2), LON + LAT)
    wide = P(None, LON, LAT)
    flat = P(LON, LAT)
    return jax.shard_map(
        body,
        mesh=torus,
        in_specs=(wide, wide, P(), flat, flat, flat, flat),
        out_specs=(flat, flat),
        check_vma=False,
    )
```

```python
import math

import jax
import jax.numpy as jnp
from jax import lax
from jax.experimental import pallas as pl
from jax.experimental.pallas import tpu as pltpu
from jax.sharding import Mesh
from jax.sharding import PartitionSpec as P

LEVELS = 40
CHUNKS = 2
ROWS = 8
COLS = 512
FIELDS = 6
REACH = 4
WIDTH = 7
EDGE = 112
MOMENTS = 122
PLAIN = 116
EDGE_COLS = 256
LON = ("lon_0", "lon_1", "lon_2")
LAT = ("lat_0", "lat_1")
NEAR = ("lon_2", "lat_0", "lat_1")
FAR = ("lon_0", "lon_1")
SCALE = 1.0 / math.sqrt(LEVELS)
VMEM = pl.BlockSpec(memory_space=pltpu.VMEM)
ANY = pl.BlockSpec(memory_space=pl.ANY)


def lon_even():
    return lax.rem(lax.axis_index("lon_2"), 2) == 0


def lat_index():
    return 2 * lax.axis_index("lat_0") + lax.axis_index("lat_1")


def pick(flag, yes, no):
    return jnp.where(jnp.full(yes.shape, flag), yes, no)


def turn(tile, lanes):
    return tile if lanes % 128 == 0 else pltpu.roll(tile, lanes % 128, 1)


def sublane(shape):
    return lax.broadcasted_iota(jnp.int32, shape, len(shape) - 2)


def lane(shape):
    return lax.broadcasted_iota(jnp.int32, shape, len(shape) - 1)


def sum_kernel(thick_in, u, v, depth, mask, damping, eta, own, odd, even, u_buf, v_buf, f_buf, m_buf, thick, sems, f_sems):
    step = LEVELS // CHUNKS
    weights = pltpu.make_async_copy(thick_in, thick, f_sems.at[4])
    weights.start()
    copies = []
    for c in range(CHUNKS):
        part = pl.ds(c * step, step)
        copies.append(
            (
                pltpu.make_async_copy(u.at[part], u_buf.at[part], sems.at[0, c]),
                pltpu.make_async_copy(v.at[part], v_buf.at[part], sems.at[1, c]),
            )
        )
    small = [
        pltpu.make_async_copy(depth, f_buf.at[0], f_sems.at[0]),
        pltpu.make_async_copy(damping, f_buf.at[1], f_sems.at[1]),
        pltpu.make_async_copy(eta, f_buf.at[2], f_sems.at[2]),
        pltpu.make_async_copy(mask, m_buf, f_sems.at[3]),
    ]
    for a, b in copies:
        a.start()
        b.start()
    for s in small:
        s.start()
    total = [jnp.zeros((ROWS, COLS), jnp.float32), jnp.zeros((ROWS, COLS), jnp.float32)]
    weights.wait()
    for c in range(CHUNKS):
        for i, buf in enumerate((u_buf, v_buf)):
            copies[c][i].wait()
            for k in range(c * step, (c + 1) * step):
                total[i] = total[i] + thick[k] * buf[k]
    for s in small:
        s.wait()
    wet = m_buf[...].astype(jnp.float32)
    fields = [total[0] * SCALE, total[1] * SCALE, f_buf[0], wet, f_buf[1], f_buf[2]]
    for i, field in enumerate(fields):
        own[i] = field
    high = sublane((ROWS, COLS)) >= ROWS // 2
    flag = lon_even()
    for p in range(FIELDS // 2):
        a, b = fields[2 * p], pltpu.roll(fields[2 * p + 1], ROWS // 2, 0)
        first = jnp.where(high, b, a)
        last = jnp.where(high, a, b)
        even[p] = pick(flag, last, first)
        odd[p] = pick(flag, first, last)


def stencil(face_x, face_y, rhs, diag):
    rows, cols = rhs.shape
    back_x, back_y = pltpu.roll(face_x, 1, 0), pltpu.roll(face_y, 1, 1)
    diag = jnp.where(diag > 0.0, diag, 1.0)

    def spread(a):
        ends = face_x * pltpu.roll(a, rows - 1, 0) + back_x * pltpu.roll(a, 1, 0)
        return ends + face_y * pltpu.roll(a, cols - 1, 1) + back_y * pltpu.roll(a, 1, 1)

    w0 = rhs
    v0 = w0 / diag
    w1 = diag * v0 - spread(v0)
    v1 = w1 / diag
    w2 = -spread(v1)
    v2 = w2 / diag
    w3 = -spread(v2)
    return [a[:ROWS] for a in (v0, v1, v2, w0, w1, w2, w3)]


def add_moments(basis, keep):
    s0, s1, s2, w0, w1, w2, w3 = basis
    n1, n2 = s0 - s1, s0 - s1 + s2
    m1 = w0 - w1
    m2 = m1 + w2
    m3 = m2 - w3
    plain = ((s0, m1), (n1, m1), (n1, m2), (n2, m2), (n2, m3))
    newton = ((s0, w0), (s0, w1), (s1, w1), (s1, w2), (s2, w2), (s2, w3))
    row = jnp.zeros((1, 128), jnp.float32)
    spot = lane((1, 128))
    for at, (a, b) in (*enumerate(plain, PLAIN), *enumerate(newton, MOMENTS)):
        prod = jnp.where(keep, a * b, 0.0)
        tiles = [prod[:, i : i + 128] for i in range(0, prod.shape[1], 128)]
        while len(tiles) > 1:
            tiles = [tiles[i] + tiles[i + 1] for i in range(0, len(tiles), 2)]
        total = jnp.sum(jnp.sum(tiles[0], axis=0, keepdims=True), axis=1, keepdims=True)
        row = jnp.where(spot == at, total, row)
    return row


def block_kernel(own, got_odd, got_even, basis, slots):
    flag = lon_even()
    high = sublane((ROWS, COLS)) >= ROWS // 2
    rows = []
    for p in range(FIELDS // 2):
        above = pick(flag, got_even[p], got_odd[p])
        below = pick(flag, got_odd[p], got_even[p])
        rows.append(jnp.where(high, below, above))
        rows.append(pltpu.roll(jnp.where(high, above, below), ROWS // 2, 0))
    fields = [jnp.concatenate([own[i], rows[i]], axis=0) for i in range(FIELDS)]
    sum_east, sum_north, depth, wet, damping, eta = fields
    inner = lane(wet.shape) < COLS - 1
    wet_x = wet * pltpu.roll(wet, 2 * ROWS - 1, 0)
    wet_y = jnp.where(inner, wet * pltpu.roll(wet, COLS - 1, 1), 0.0)
    face_x = wet_x * 0.5 * (depth + pltpu.roll(depth, 2 * ROWS - 1, 0))
    face_y = wet_y * 0.5 * (depth + pltpu.roll(depth, COLS - 1, 1))
    flux_x = wet_x * sum_east
    flux_y = wet_y * sum_north
    diverge = flux_x - pltpu.roll(flux_x, 1, 0) + flux_y - pltpu.roll(flux_y, 1, 1)
    rhs = wet * (damping * eta - diverge)
    diag = damping + face_x + pltpu.roll(face_x, 1, 0) + face_y + pltpu.roll(face_y, 1, 1)
    parts = stencil(face_x, face_y, rhs, diag)
    for i, part in enumerate(parts):
        basis[i] = part
    place = lat_index()
    spot = lane((ROWS, COLS))
    low = jnp.where(place == 0, 0, REACH)
    top = jnp.where(place == lax.axis_size(LAT) - 1, COLS, COLS - REACH)
    keep = jnp.logical_and(spot >= low, spot < top)
    row = jnp.broadcast_to(add_moments(parts, keep), (ROWS, 128))
    spot = lane((ROWS, 128))
    deep = sublane((ROWS, 128))
    tile = jnp.where(deep == 0, row, jnp.where(deep == 1, turn(row, MOMENTS - PLAIN), 0.0))
    pieces = []
    for t in range(2):
        for i, field in enumerate((rhs, diag, face_x, face_y)):
            at = 2 * WIDTH * (4 * t + i)
            pieces.append((field, t, COLS - WIDTH, at, WIDTH))
            pieces.append((field, t, 0, at + WIDTH, WIDTH))
        for i, field in enumerate((wet, depth, sum_north)):
            pieces.append((field, t, COLS - 1, EDGE + 2 * i + t, 1))
        for i, field in enumerate((wet, depth)):
            pieces.append((field, t, 0, EDGE + 6 + 2 * i + t, 1))
    for field, t, start, at, size in pieces:
        base = start - start % 128
        moved = turn(field[ROWS * t : ROWS * (t + 1), base : base + 128], at - start % 128)
        tile = jnp.where(jnp.logical_and(spot >= at, spot < at + size), moved, tile)
    for i in range(slots.shape[0]):
        slots[i] = tile


def edge_kernel(slots, edge_basis, moments):
    spot = lane((ROWS, 128))
    count = lax.axis_size(LAT)
    group = slots.shape[0]
    left = jnp.logical_and(spot < EDGE, lax.rem(spot, 2 * WIDTH) < WIDTH)
    left = jnp.logical_or(left, jnp.logical_and(spot >= EDGE, spot < EDGE + 6))
    tiles = EDGE_COLS // 128
    zero = jnp.zeros((ROWS, 128), jnp.float32)
    fields = [[[zero for _ in range(tiles)] for _ in range(2)] for _ in range(6)]
    for b in range(group // count * (count - 1)):
        slot = b // (count - 1) * count + b % (count - 1)
        pair = jnp.where(left, slots[slot], slots[slot + 1])
        far = turn(pair, -6)
        wets = pair * far
        face = wets * 0.5 * turn(pair + far, -2)
        flux = wets * turn(pair, -4)
        at, home = 16 * (b % 8), b // 8
        here = jnp.logical_and(spot >= at, spot < at + 2 * WIDTH)
        seam = spot == at + WIDTH - 1
        for t in range(2):
            for i in range(4):
                moved = turn(pair, at - 2 * WIDTH * (4 * t + i))
                fields[i][t][home] = jnp.where(here, moved, fields[i][t][home])
            for i, value in enumerate((face, flux)):
                moved = turn(value, at + WIDTH - 1 - EDGE - t)
                fields[4 + i][t][home] = jnp.where(seam, moved, fields[4 + i][t][home])
    fields = [jnp.concatenate([jnp.concatenate(f[t], axis=1) for t in range(2)], axis=0) for f in fields]
    rhs, diag, face_x, face_y, face, flux = fields
    rhs = rhs - flux + pltpu.roll(flux, 1, 1)
    diag = diag + face + pltpu.roll(face, 1, 1)
    face_y = face_y + face
    parts = stencil(face_x, face_y, rhs, diag)
    for i, part in enumerate(parts):
        edge_basis[i] = part
    spot = lane((ROWS, EDGE_COLS))
    column = lax.rem(spot, 16)
    keep = jnp.logical_and(column >= WIDTH - REACH, column < WIDTH + REACH)
    row = add_moments(parts, keep)
    sums = [slots[i] for i in range(group)]
    while len(sums) > 1:
        sums = [sums[i] + sums[i + 1] for i in range(0, len(sums), 2)]
    total = jnp.where(lane((ROWS, 128)) >= MOMENTS, sums[0], pltpu.roll(turn(sums[0], PLAIN - MOMENTS), ROWS - 1, 0))
    moments[...] = jnp.broadcast_to(total[:1] + row, moments.shape)


def poly(a, b, scale):
    size = max(len(a), len(b))
    out = []
    for i in range(size):
        if i >= len(b):
            out.append(a[i])
        elif i >= len(a):
            out.append(scale * b[i])
        else:
            out.append(a[i] + scale * b[i])
    return out


def square(a, gram):
    total = None
    for i in range(len(a)):
        for j in range(i, len(a)):
            term = a[i] * a[j] * gram[i, j]
            term = term if i == j else 2.0 * term
            total = term if total is None else total + term
    return total


def final_kernel(parts, basis, edge_basis, surface, residual):
    row = jnp.sum(parts[...], axis=0, keepdims=True)
    spot = lane((1, 128))
    def at(k):
        return jnp.sum(jnp.where(spot == k, row, 0.0), axis=1, keepdims=True)

    g00, g01, g11, g12, g22, g23 = [at(MOMENTS + k) for k in range(6)]
    m1, m2, m3, m4, m5 = [at(PLAIN + k) for k in range(5)]
    rough = g01 > 0.5 * g00
    newton = {(0, 0): g00, (0, 1): g01, (1, 1): g11, (0, 2): g11 - g01, (1, 2): g12, (2, 2): g22}
    plain = {(0, 0): g00, (0, 1): m1, (1, 1): m2, (0, 2): m2, (1, 2): m3, (2, 2): m4}
    gram = {k: jnp.where(rough, plain[k], newton[k]) for k in plain}
    newton = {(0, 0): g01, (0, 1): g11, (1, 1): g12 + g11, (0, 2): g12, (1, 2): g22 + g12, (2, 2): g23 + g22}
    plain = {(0, 0): g00 - m1, (0, 1): m1 - m2, (1, 1): m2 - m3, (0, 2): m2 - m3, (1, 2): m3 - m4, (2, 2): m4 - m5}
    energy = {k: jnp.where(rough, plain[k], newton[k]) for k in plain}
    stay, shift = jnp.where(rough, 1.0, 0.0), jnp.where(rough, -1.0, 1.0)
    one = jnp.ones((1, 1), jnp.float32)
    pre, direction = [one], [one]
    gamma = g00
    step = gamma / energy[0, 0]
    answer = [step]
    for sweep in range(3):
        image = [stay * direction[0]]
        for i in range(1, sweep + 1):
            image.append(direction[i] + shift * direction[i - 1])
        image.append(shift * direction[-1])
        pre = poly(pre, image, -step)
        if sweep == 2:
            break
        gamma_next = square(pre, gram)
        delta = square(pre, energy)
        ratio = gamma_next / gamma
        step = gamma_next / (delta - ratio * gamma_next / step)
        direction = poly(pre, direction, ratio)
        answer = poly(answer, direction, step)
        gamma = gamma_next
    for coefs in (answer, pre):
        for i in range(len(coefs) - 1, 0, -1):
            coefs[i - 1] = coefs[i - 1] + jnp.where(rough, coefs[i], 0.0)
        for i in range(1, len(coefs), 2):
            coefs[i] = shift * coefs[i]

    def combine(b):
        eta = answer[0] * b[0] + answer[1] * b[1] + answer[2] * b[2]
        return eta, (pre[0] * b[3] + pre[1] * b[4]) + (pre[2] * b[5] + pre[3] * b[6])

    inner, edge = combine(basis), combine(edge_basis)
    place, count = lat_index(), lax.axis_size(LAT)
    group = lax.axis_index("lon_2") * (count - 1)
    spot = lane((ROWS, 128))
    for out, body, strip in ((surface, inner[0], edge[0]), (residual, inner[1], edge[1])):
        out[:, 128 : COLS - 128] = body[:, 128 : COLS - 128]
        for side, ok, base, near in ((-1, place > 0, 0, spot < REACH), (0, place < count - 1, COLS - 128, spot >= 128 - REACH)):
            b = group + place + side
            tile = strip[:, :128]
            for i in range(1, EDGE_COLS // 128):
                tile = pick(b // 8 == i, strip[:, 128 * i : 128 * (i + 1)], tile)
            start = 16 * lax.rem(b, 8) + WIDTH
            moved = pltpu.roll(tile, lax.rem(256 - start, 128), 1)
            use = jnp.logical_and(near, ok)
            out[:, base : base + 128] = jnp.where(use, moved, body[:, base : base + 128])


def kept(*dims):
    return pltpu.VMEM(dims, jnp.float32)


def shape(*dims):
    return jax.ShapeDtypeStruct(dims, jnp.float32)


def call(kernel, name, outs, *args):
    args = [pltpu.with_memory_space_constraint(a, pltpu.VMEM) for a in args]
    specs = jax.tree.map(lambda _: VMEM, outs)
    return pl.pallas_call(kernel, out_shape=outs, in_specs=[VMEM] * len(args), out_specs=specs, name=name)(*args)


def body(u_vel, v_vel, thickness, depth, sea_mask, damping, eta_prev):
    count = lax.axis_size(LON)
    pairs_even = [(i, i ^ 1) for i in range(count)]
    pairs_odd = [(i, (i + 1) % count) if i % 2 else (i, (i - 1) % count) for i in range(count)]
    own, odd, even = pl.pallas_call(
        sum_kernel,
        out_shape=(kept(FIELDS, ROWS, COLS), kept(3, ROWS, COLS), kept(3, ROWS, COLS)),
        in_specs=[ANY] * 7,
        out_specs=(VMEM, VMEM, VMEM),
        scratch_shapes=[
            pltpu.VMEM((LEVELS, ROWS, COLS), jnp.float32),
            pltpu.VMEM((LEVELS, ROWS, COLS), jnp.float32),
            pltpu.VMEM((3, ROWS, COLS), jnp.float32),
            pltpu.VMEM((ROWS, COLS), jnp.int32),
            pltpu.SMEM((LEVELS,), jnp.float32),
            pltpu.SemaphoreType.DMA((2, CHUNKS)),
            pltpu.SemaphoreType.DMA((5,)),
        ],
        name="sums",
    )(thickness, u_vel, v_vel, depth, sea_mask, damping, eta_prev)
    got_odd = lax.ppermute(odd, LON, pairs_odd)
    got_even = lax.ppermute(even, LON, pairs_even)
    near, far = lax.axis_size(NEAR), lax.axis_size(FAR)
    basis, slots = call(block_kernel, "block", (kept(7, ROWS, COLS), kept(near, ROWS, 128)), own, got_odd, got_even)
    slots = lax.all_to_all(slots, NEAR, 0, 0, tiled=True)
    edge_basis, moments = call(edge_kernel, "edge", (kept(7, ROWS, EDGE_COLS), kept(far, 128)), slots)
    moments = lax.all_to_all(moments, FAR, 0, 0, tiled=True)
    outs = (shape(ROWS, COLS), shape(ROWS, COLS))
    return call(final_kernel, "final", outs, moments, basis, edge_basis)


def solution(mesh):
    torus = Mesh(mesh.devices.reshape(8, 8, 4, 2, 2), LON + LAT)
    wide = P(None, LON, LAT)
    flat = P(LON, LAT)
    return jax.shard_map(
        body,
        mesh=torus,
        in_specs=(wide, wide, P(), flat, flat, flat, flat),
        out_specs=(flat, flat),
        check_vma=False,
    )
```

```python
import math

import jax
import jax.numpy as jnp
from jax import lax
from jax.experimental import pallas as pl
from jax.experimental.pallas import tpu as pltpu
from jax.sharding import Mesh
from jax.sharding import PartitionSpec as P

LEVELS = 40
CHUNKS = 2
ROWS = 8
COLS = 512
FIELDS = 6
REACH = 4
WIDTH = 7
EDGE = 112
MOMENTS = 122
PLAIN = 116
EDGE_COLS = 256
LON = ("lon_0", "lon_1", "lon_2")
LAT = ("lat_0", "lat_1")
NEAR = ("lon_2", "lat_0", "lat_1")
FAR = ("lon_1", "lon_0")
SCALE = 1.0 / math.sqrt(LEVELS)
VMEM = pl.BlockSpec(memory_space=pltpu.VMEM)
ANY = pl.BlockSpec(memory_space=pl.ANY)


def lon_even():
    return lax.rem(lax.axis_index("lon_2"), 2) == 0


def lat_index():
    return 2 * lax.axis_index("lat_0") + lax.axis_index("lat_1")


def pick(flag, yes, no):
    return jnp.where(jnp.full(yes.shape, flag), yes, no)


def turn(tile, lanes):
    return tile if lanes % 128 == 0 else pltpu.roll(tile, lanes % 128, 1)


def sublane(shape):
    return lax.broadcasted_iota(jnp.int32, shape, len(shape) - 2)


def lane(shape):
    return lax.broadcasted_iota(jnp.int32, shape, len(shape) - 1)


def sum_kernel(thick_in, u, v, depth, mask, damping, eta, own, odd, even, u_buf, v_buf, f_buf, m_buf, thick, sems, f_sems):
    step = LEVELS // CHUNKS
    weights = pltpu.make_async_copy(thick_in, thick, f_sems.at[4])
    weights.start()
    copies = []
    for c in range(CHUNKS):
        part = pl.ds(c * step, step)
        copies.append(
            (
                pltpu.make_async_copy(u.at[part], u_buf.at[part], sems.at[0, c]),
                pltpu.make_async_copy(v.at[part], v_buf.at[part], sems.at[1, c]),
            )
        )
    small = [
        pltpu.make_async_copy(depth, f_buf.at[0], f_sems.at[0]),
        pltpu.make_async_copy(damping, f_buf.at[1], f_sems.at[1]),
        pltpu.make_async_copy(eta, f_buf.at[2], f_sems.at[2]),
        pltpu.make_async_copy(mask, m_buf, f_sems.at[3]),
    ]
    for a, b in copies:
        a.start()
        b.start()
    for s in small:
        s.start()
    total = [jnp.zeros((ROWS, COLS), jnp.float32), jnp.zeros((ROWS, COLS), jnp.float32)]
    weights.wait()
    for c in range(CHUNKS):
        for i, buf in enumerate((u_buf, v_buf)):
            copies[c][i].wait()
            for k in range(c * step, (c + 1) * step):
                total[i] = total[i] + thick[k] * buf[k]
    for s in small:
        s.wait()
    wet = m_buf[...].astype(jnp.float32)
    fields = [total[0] * SCALE, total[1] * SCALE, f_buf[0], wet, f_buf[1], f_buf[2]]
    for i, field in enumerate(fields):
        own[i] = field
    high = sublane((ROWS, COLS)) >= ROWS // 2
    flag = lon_even()
    for p in range(FIELDS // 2):
        a, b = fields[2 * p], pltpu.roll(fields[2 * p + 1], ROWS // 2, 0)
        first = jnp.where(high, b, a)
        last = jnp.where(high, a, b)
        even[p] = pick(flag, last, first)
        odd[p] = pick(flag, first, last)


def stencil(face_x, face_y, rhs, diag):
    rows, cols = rhs.shape
    back_x, back_y = pltpu.roll(face_x, 1, 0), pltpu.roll(face_y, 1, 1)
    diag = jnp.where(diag > 0.0, diag, 1.0)

    def spread(a):
        ends = face_x * pltpu.roll(a, rows - 1, 0) + back_x * pltpu.roll(a, 1, 0)
        return ends + face_y * pltpu.roll(a, cols - 1, 1) + back_y * pltpu.roll(a, 1, 1)

    w0 = rhs
    v0 = w0 / diag
    w1 = diag * v0 - spread(v0)
    v1 = w1 / diag
    w2 = -spread(v1)
    v2 = w2 / diag
    w3 = -spread(v2)
    return [a[:ROWS] for a in (v0, v1, v2, w0, w1, w2, w3)]


def add_moments(basis, keep):
    s0, s1, s2, w0, w1, w2, w3 = basis
    n1, n2 = s0 - s1, s0 - s1 + s2
    m1 = w0 - w1
    m2 = m1 + w2
    m3 = m2 - w3
    plain = ((s0, m1), (n1, m1), (n1, m2), (n2, m2), (n2, m3))
    newton = ((s0, w0), (s0, w1), (s1, w1), (s1, w2), (s2, w2), (s2, w3))
    row = jnp.zeros((1, 128), jnp.float32)
    spot = lane((1, 128))
    for at, (a, b) in (*enumerate(plain, PLAIN), *enumerate(newton, MOMENTS)):
        prod = jnp.where(keep, a * b, 0.0)
        tiles = [prod[:, i : i + 128] for i in range(0, prod.shape[1], 128)]
        while len(tiles) > 1:
            tiles = [tiles[i] + tiles[i + 1] for i in range(0, len(tiles), 2)]
        total = jnp.sum(jnp.sum(tiles[0], axis=0, keepdims=True), axis=1, keepdims=True)
        row = jnp.where(spot == at, total, row)
    return row


def block_kernel(own, got_odd, got_even, basis, slots):
    flag = lon_even()
    high = sublane((ROWS, COLS)) >= ROWS // 2
    rows = []
    for p in range(FIELDS // 2):
        above = pick(flag, got_even[p], got_odd[p])
        below = pick(flag, got_odd[p], got_even[p])
        rows.append(jnp.where(high, below, above))
        rows.append(pltpu.roll(jnp.where(high, above, below), ROWS // 2, 0))
    fields = [jnp.concatenate([own[i], rows[i]], axis=0) for i in range(FIELDS)]
    sum_east, sum_north, depth, wet, damping, eta = fields
    inner = lane(wet.shape) < COLS - 1
    wet_x = wet * pltpu.roll(wet, 2 * ROWS - 1, 0)
    wet_y = jnp.where(inner, wet * pltpu.roll(wet, COLS - 1, 1), 0.0)
    face_x = wet_x * 0.5 * (depth + pltpu.roll(depth, 2 * ROWS - 1, 0))
    face_y = wet_y * 0.5 * (depth + pltpu.roll(depth, COLS - 1, 1))
    flux_x = wet_x * sum_east
    flux_y = wet_y * sum_north
    diverge = flux_x - pltpu.roll(flux_x, 1, 0) + flux_y - pltpu.roll(flux_y, 1, 1)
    rhs = wet * (damping * eta - diverge)
    diag = damping + face_x + pltpu.roll(face_x, 1, 0) + face_y + pltpu.roll(face_y, 1, 1)
    parts = stencil(face_x, face_y, rhs, diag)
    for i, part in enumerate(parts):
        basis[i] = part
    place = lat_index()
    spot = lane((ROWS, COLS))
    low = jnp.where(place == 0, 0, REACH)
    top = jnp.where(place == lax.axis_size(LAT) - 1, COLS, COLS - REACH)
    keep = jnp.logical_and(spot >= low, spot < top)
    row = jnp.broadcast_to(add_moments(parts, keep), (ROWS, 128))
    spot = lane((ROWS, 128))
    deep = sublane((ROWS, 128))
    tile = jnp.where(deep == 0, row, jnp.where(deep == 1, turn(row, MOMENTS - PLAIN), 0.0))
    pieces = []
    for t in range(2):
        for i, field in enumerate((rhs, diag, face_x, face_y)):
            at = 2 * WIDTH * (4 * t + i)
            pieces.append((field, t, COLS - WIDTH, at, WIDTH))
            pieces.append((field, t, 0, at + WIDTH, WIDTH))
        for i, field in enumerate((wet, depth, sum_north)):
            pieces.append((field, t, COLS - 1, EDGE + 2 * i + t, 1))
        for i, field in enumerate((wet, depth)):
            pieces.append((field, t, 0, EDGE + 6 + 2 * i + t, 1))
    for field, t, start, at, size in pieces:
        base = start - start % 128
        moved = turn(field[ROWS * t : ROWS * (t + 1), base : base + 128], at - start % 128)
        tile = jnp.where(jnp.logical_and(spot >= at, spot < at + size), moved, tile)
    for i in range(slots.shape[0]):
        slots[i] = tile


def edge_kernel(slots, edge_basis, moments):
    spot = lane((ROWS, 128))
    count = lax.axis_size(LAT)
    group = slots.shape[0]
    left = jnp.logical_and(spot < EDGE, lax.rem(spot, 2 * WIDTH) < WIDTH)
    left = jnp.logical_or(left, jnp.logical_and(spot >= EDGE, spot < EDGE + 6))
    tiles = EDGE_COLS // 128
    zero = jnp.zeros((ROWS, 128), jnp.float32)
    fields = [[[zero for _ in range(tiles)] for _ in range(2)] for _ in range(6)]
    for b in range(group // count * (count - 1)):
        slot = b // (count - 1) * count + b % (count - 1)
        pair = jnp.where(left, slots[slot], slots[slot + 1])
        far = turn(pair, -6)
        wets = pair * far
        face = wets * 0.5 * turn(pair + far, -2)
        flux = wets * turn(pair, -4)
        at, home = 16 * (b % 8), b // 8
        here = jnp.logical_and(spot >= at, spot < at + 2 * WIDTH)
        seam = spot == at + WIDTH - 1
        for t in range(2):
            for i in range(4):
                moved = turn(pair, at - 2 * WIDTH * (4 * t + i))
                fields[i][t][home] = jnp.where(here, moved, fields[i][t][home])
            for i, value in enumerate((face, flux)):
                moved = turn(value, at + WIDTH - 1 - EDGE - t)
                fields[4 + i][t][home] = jnp.where(seam, moved, fields[4 + i][t][home])
    fields = [jnp.concatenate([jnp.concatenate(f[t], axis=1) for t in range(2)], axis=0) for f in fields]
    rhs, diag, face_x, face_y, face, flux = fields
    rhs = rhs - flux + pltpu.roll(flux, 1, 1)
    diag = diag + face + pltpu.roll(face, 1, 1)
    face_y = face_y + face
    parts = stencil(face_x, face_y, rhs, diag)
    for i, part in enumerate(parts):
        edge_basis[i] = part
    spot = lane((ROWS, EDGE_COLS))
    column = lax.rem(spot, 16)
    keep = jnp.logical_and(column >= WIDTH - REACH, column < WIDTH + REACH)
    row = add_moments(parts, keep)
    sums = [slots[i] for i in range(group)]
    while len(sums) > 1:
        sums = [sums[i] + sums[i + 1] for i in range(0, len(sums), 2)]
    total = jnp.where(lane((ROWS, 128)) >= MOMENTS, sums[0], pltpu.roll(turn(sums[0], PLAIN - MOMENTS), ROWS - 1, 0))
    moments[...] = jnp.broadcast_to(total[:1] + row, moments.shape)


def poly(a, b, scale):
    size = max(len(a), len(b))
    out = []
    for i in range(size):
        if i >= len(b):
            out.append(a[i])
        elif i >= len(a):
            out.append(scale * b[i])
        else:
            out.append(a[i] + scale * b[i])
    return out


def square(a, gram):
    total = None
    for i in range(len(a)):
        for j in range(i, len(a)):
            term = a[i] * a[j] * gram[i, j]
            term = term if i == j else 2.0 * term
            total = term if total is None else total + term
    return total


def final_kernel(parts, basis, edge_basis, surface, residual):
    row = jnp.sum(parts[...], axis=0, keepdims=True)
    spot = lane((1, 128))
    def at(k):
        return jnp.sum(jnp.where(spot == k, row, 0.0), axis=1, keepdims=True)

    g00, g01, g11, g12, g22, g23 = [at(MOMENTS + k) for k in range(6)]
    m1, m2, m3, m4, m5 = [at(PLAIN + k) for k in range(5)]
    rough = g01 > 0.5 * g00
    newton = {(0, 0): g00, (0, 1): g01, (1, 1): g11, (0, 2): g11 - g01, (1, 2): g12, (2, 2): g22}
    plain = {(0, 0): g00, (0, 1): m1, (1, 1): m2, (0, 2): m2, (1, 2): m3, (2, 2): m4}
    gram = {k: jnp.where(rough, plain[k], newton[k]) for k in plain}
    newton = {(0, 0): g01, (0, 1): g11, (1, 1): g12 + g11, (0, 2): g12, (1, 2): g22 + g12, (2, 2): g23 + g22}
    plain = {(0, 0): g00 - m1, (0, 1): m1 - m2, (1, 1): m2 - m3, (0, 2): m2 - m3, (1, 2): m3 - m4, (2, 2): m4 - m5}
    energy = {k: jnp.where(rough, plain[k], newton[k]) for k in plain}
    stay, shift = jnp.where(rough, 1.0, 0.0), jnp.where(rough, -1.0, 1.0)
    one = jnp.ones((1, 1), jnp.float32)
    pre, direction = [one], [one]
    gamma = g00
    step = gamma / energy[0, 0]
    answer = [step]
    for sweep in range(3):
        image = [stay * direction[0]]
        for i in range(1, sweep + 1):
            image.append(direction[i] + shift * direction[i - 1])
        image.append(shift * direction[-1])
        pre = poly(pre, image, -step)
        if sweep == 2:
            break
        gamma_next = square(pre, gram)
        delta = square(pre, energy)
        ratio = gamma_next / gamma
        step = gamma_next / (delta - ratio * gamma_next / step)
        direction = poly(pre, direction, ratio)
        answer = poly(answer, direction, step)
        gamma = gamma_next
    for coefs in (answer, pre):
        for i in range(len(coefs) - 1, 0, -1):
            coefs[i - 1] = coefs[i - 1] + jnp.where(rough, coefs[i], 0.0)
        for i in range(1, len(coefs), 2):
            coefs[i] = shift * coefs[i]

    def combine(b):
        eta = answer[0] * b[0] + answer[1] * b[1] + answer[2] * b[2]
        return eta, (pre[0] * b[3] + pre[1] * b[4]) + (pre[2] * b[5] + pre[3] * b[6])

    inner, edge = combine(basis), combine(edge_basis)
    place, count = lat_index(), lax.axis_size(LAT)
    group = lax.axis_index("lon_2") * (count - 1)
    spot = lane((ROWS, 128))
    for out, body, strip in ((surface, inner[0], edge[0]), (residual, inner[1], edge[1])):
        out[:, 128 : COLS - 128] = body[:, 128 : COLS - 128]
        for side, ok, base, near in ((-1, place > 0, 0, spot < REACH), (0, place < count - 1, COLS - 128, spot >= 128 - REACH)):
            b = group + place + side
            tile = strip[:, :128]
            for i in range(1, EDGE_COLS // 128):
                tile = pick(b // 8 == i, strip[:, 128 * i : 128 * (i + 1)], tile)
            start = 16 * lax.rem(b, 8) + WIDTH
            moved = pltpu.roll(tile, lax.rem(256 - start, 128), 1)
            use = jnp.logical_and(near, ok)
            out[:, base : base + 128] = jnp.where(use, moved, body[:, base : base + 128])


def kept(*dims):
    return pltpu.VMEM(dims, jnp.float32)


def shape(*dims):
    return jax.ShapeDtypeStruct(dims, jnp.float32)


def call(kernel, name, outs, *args):
    args = [pltpu.with_memory_space_constraint(a, pltpu.VMEM) for a in args]
    specs = jax.tree.map(lambda _: VMEM, outs)
    return pl.pallas_call(kernel, out_shape=outs, in_specs=[VMEM] * len(args), out_specs=specs, name=name)(*args)


def body(u_vel, v_vel, thickness, depth, sea_mask, damping, eta_prev):
    count = lax.axis_size(LON)
    pairs_even = [(i, i ^ 1) for i in range(count)]
    pairs_odd = [(i, (i + 1) % count) if i % 2 else (i, (i - 1) % count) for i in range(count)]
    own, odd, even = pl.pallas_call(
        sum_kernel,
        out_shape=(kept(FIELDS, ROWS, COLS), kept(3, ROWS, COLS), kept(3, ROWS, COLS)),
        in_specs=[ANY] * 7,
        out_specs=(VMEM, VMEM, VMEM),
        scratch_shapes=[
            pltpu.VMEM((LEVELS, ROWS, COLS), jnp.float32),
            pltpu.VMEM((LEVELS, ROWS, COLS), jnp.float32),
            pltpu.VMEM((3, ROWS, COLS), jnp.float32),
            pltpu.VMEM((ROWS, COLS), jnp.int32),
            pltpu.SMEM((LEVELS,), jnp.float32),
            pltpu.SemaphoreType.DMA((2, CHUNKS)),
            pltpu.SemaphoreType.DMA((5,)),
        ],
        name="sums",
    )(thickness, u_vel, v_vel, depth, sea_mask, damping, eta_prev)
    got_odd = lax.ppermute(odd, LON, pairs_odd)
    got_even = lax.ppermute(even, LON, pairs_even)
    near, far = lax.axis_size(NEAR), lax.axis_size(FAR)
    basis, slots = call(block_kernel, "block", (kept(7, ROWS, COLS), kept(near, ROWS, 128)), own, got_odd, got_even)
    slots = lax.all_to_all(slots, NEAR, 0, 0, tiled=True)
    edge_basis, moments = call(edge_kernel, "edge", (kept(7, ROWS, EDGE_COLS), kept(far, 128)), slots)
    moments = lax.all_to_all(moments, FAR, 0, 0, tiled=True)
    outs = (shape(ROWS, COLS), shape(ROWS, COLS))
    return call(final_kernel, "final", outs, moments, basis, edge_basis)


def solution(mesh):
    torus = Mesh(mesh.devices.reshape(8, 8, 4, 2, 2), LON + LAT)
    wide = P(None, LON, LAT)
    flat = P(LON, LAT)
    return jax.shard_map(
        body,
        mesh=torus,
        in_specs=(wide, wide, P(), flat, flat, flat, flat),
        out_specs=(flat, flat),
        check_vma=False,
    )
```

```python
import math

import jax
import jax.numpy as jnp
from jax import lax
from jax.experimental import pallas as pl
from jax.experimental.pallas import tpu as pltpu
from jax.sharding import Mesh
from jax.sharding import PartitionSpec as P

LEVELS = 40
CHUNKS = 1
ROWS = 8
COLS = 512
FIELDS = 6
REACH = 4
WIDTH = 7
EDGE = 112
MOMENTS = 122
PLAIN = 116
EDGE_COLS = 256
LON = ("lon_0", "lon_1", "lon_2")
LAT = ("lat_0", "lat_1")
NEAR = ("lon_2", "lat_0", "lat_1")
FAR = ("lon_0", "lon_1")
SCALE = 1.0 / math.sqrt(LEVELS)
VMEM = pl.BlockSpec(memory_space=pltpu.VMEM)
ANY = pl.BlockSpec(memory_space=pl.ANY)


def lon_even():
    return lax.rem(lax.axis_index("lon_2"), 2) == 0


def lat_index():
    return 2 * lax.axis_index("lat_0") + lax.axis_index("lat_1")


def pick(flag, yes, no):
    return jnp.where(jnp.full(yes.shape, flag), yes, no)


def turn(tile, lanes):
    return tile if lanes % 128 == 0 else pltpu.roll(tile, lanes % 128, 1)


def sublane(shape):
    return lax.broadcasted_iota(jnp.int32, shape, len(shape) - 2)


def lane(shape):
    return lax.broadcasted_iota(jnp.int32, shape, len(shape) - 1)


def sum_kernel(thick_in, u, v, depth, mask, damping, eta, own, odd, even, u_buf, v_buf, f_buf, m_buf, thick, sems, f_sems):
    step = LEVELS // CHUNKS
    weights = pltpu.make_async_copy(thick_in, thick, f_sems.at[4])
    weights.start()
    copies = []
    for c in range(CHUNKS):
        part = pl.ds(c * step, step)
        copies.append(
            (
                pltpu.make_async_copy(u.at[part], u_buf.at[part], sems.at[0, c]),
                pltpu.make_async_copy(v.at[part], v_buf.at[part], sems.at[1, c]),
            )
        )
    small = [
        pltpu.make_async_copy(depth, f_buf.at[0], f_sems.at[0]),
        pltpu.make_async_copy(damping, f_buf.at[1], f_sems.at[1]),
        pltpu.make_async_copy(eta, f_buf.at[2], f_sems.at[2]),
        pltpu.make_async_copy(mask, m_buf, f_sems.at[3]),
    ]
    for a, b in copies:
        a.start()
        b.start()
    for s in small:
        s.start()
    total = [jnp.zeros((ROWS, COLS), jnp.float32), jnp.zeros((ROWS, COLS), jnp.float32)]
    weights.wait()
    for c in range(CHUNKS):
        for i, buf in enumerate((u_buf, v_buf)):
            copies[c][i].wait()
            for k in range(c * step, (c + 1) * step):
                total[i] = total[i] + thick[k] * buf[k]
    for s in small:
        s.wait()
    wet = m_buf[...].astype(jnp.float32)
    fields = [total[0] * SCALE, total[1] * SCALE, f_buf[0], wet, f_buf[1], f_buf[2]]
    for i, field in enumerate(fields):
        own[i] = field
    high = sublane((ROWS, COLS)) >= ROWS // 2
    flag = lon_even()
    for p in range(FIELDS // 2):
        a, b = fields[2 * p], pltpu.roll(fields[2 * p + 1], ROWS // 2, 0)
        first = jnp.where(high, b, a)
        last = jnp.where(high, a, b)
        even[p] = pick(flag, last, first)
        odd[p] = pick(flag, first, last)


def stencil(face_x, face_y, rhs, diag):
    rows, cols = rhs.shape
    back_x, back_y = pltpu.roll(face_x, 1, 0), pltpu.roll(face_y, 1, 1)
    diag = jnp.where(diag > 0.0, diag, 1.0)

    def spread(a):
        ends = face_x * pltpu.roll(a, rows - 1, 0) + back_x * pltpu.roll(a, 1, 0)
        return ends + face_y * pltpu.roll(a, cols - 1, 1) + back_y * pltpu.roll(a, 1, 1)

    w0 = rhs
    v0 = w0 / diag
    w1 = diag * v0 - spread(v0)
    v1 = w1 / diag
    w2 = -spread(v1)
    v2 = w2 / diag
    w3 = -spread(v2)
    return [a[:ROWS] for a in (v0, v1, v2, w0, w1, w2, w3)]


def add_moments(basis, keep):
    s0, s1, s2, w0, w1, w2, w3 = basis
    n1, n2 = s0 - s1, s0 - s1 + s2
    m1 = w0 - w1
    m2 = m1 + w2
    m3 = m2 - w3
    plain = ((s0, m1), (n1, m1), (n1, m2), (n2, m2), (n2, m3))
    newton = ((s0, w0), (s0, w1), (s1, w1), (s1, w2), (s2, w2), (s2, w3))
    row = jnp.zeros((1, 128), jnp.float32)
    spot = lane((1, 128))
    for at, (a, b) in (*enumerate(plain, PLAIN), *enumerate(newton, MOMENTS)):
        prod = jnp.where(keep, a * b, 0.0)
        tiles = [prod[:, i : i + 128] for i in range(0, prod.shape[1], 128)]
        while len(tiles) > 1:
            tiles = [tiles[i] + tiles[i + 1] for i in range(0, len(tiles), 2)]
        total = jnp.sum(jnp.sum(tiles[0], axis=0, keepdims=True), axis=1, keepdims=True)
        row = jnp.where(spot == at, total, row)
    return row


def block_kernel(own, got_odd, got_even, basis, slots):
    flag = lon_even()
    high = sublane((ROWS, COLS)) >= ROWS // 2
    rows = []
    for p in range(FIELDS // 2):
        above = pick(flag, got_even[p], got_odd[p])
        below = pick(flag, got_odd[p], got_even[p])
        rows.append(jnp.where(high, below, above))
        rows.append(pltpu.roll(jnp.where(high, above, below), ROWS // 2, 0))
    fields = [jnp.concatenate([own[i], rows[i]], axis=0) for i in range(FIELDS)]
    sum_east, sum_north, depth, wet, damping, eta = fields
    inner = lane(wet.shape) < COLS - 1
    wet_x = wet * pltpu.roll(wet, 2 * ROWS - 1, 0)
    wet_y = jnp.where(inner, wet * pltpu.roll(wet, COLS - 1, 1), 0.0)
    face_x = wet_x * 0.5 * (depth + pltpu.roll(depth, 2 * ROWS - 1, 0))
    face_y = wet_y * 0.5 * (depth + pltpu.roll(depth, COLS - 1, 1))
    flux_x = wet_x * sum_east
    flux_y = wet_y * sum_north
    diverge = flux_x - pltpu.roll(flux_x, 1, 0) + flux_y - pltpu.roll(flux_y, 1, 1)
    rhs = wet * (damping * eta - diverge)
    diag = damping + face_x + pltpu.roll(face_x, 1, 0) + face_y + pltpu.roll(face_y, 1, 1)
    parts = stencil(face_x, face_y, rhs, diag)
    for i, part in enumerate(parts):
        basis[i] = part
    place = lat_index()
    spot = lane((ROWS, COLS))
    low = jnp.where(place == 0, 0, REACH)
    top = jnp.where(place == lax.axis_size(LAT) - 1, COLS, COLS - REACH)
    keep = jnp.logical_and(spot >= low, spot < top)
    row = jnp.broadcast_to(add_moments(parts, keep), (ROWS, 128))
    spot = lane((ROWS, 128))
    deep = sublane((ROWS, 128))
    tile = jnp.where(deep == 0, row, jnp.where(deep == 1, turn(row, MOMENTS - PLAIN), 0.0))
    pieces = []
    for t in range(2):
        for i, field in enumerate((rhs, diag, face_x, face_y)):
            at = 2 * WIDTH * (4 * t + i)
            pieces.append((field, t, COLS - WIDTH, at, WIDTH))
            pieces.append((field, t, 0, at + WIDTH, WIDTH))
        for i, field in enumerate((wet, depth, sum_north)):
            pieces.append((field, t, COLS - 1, EDGE + 2 * i + t, 1))
        for i, field in enumerate((wet, depth)):
            pieces.append((field, t, 0, EDGE + 6 + 2 * i + t, 1))
    for field, t, start, at, size in pieces:
        base = start - start % 128
        moved = turn(field[ROWS * t : ROWS * (t + 1), base : base + 128], at - start % 128)
        tile = jnp.where(jnp.logical_and(spot >= at, spot < at + size), moved, tile)
    for i in range(slots.shape[0]):
        slots[i] = tile


def edge_kernel(slots, edge_basis, moments):
    spot = lane((ROWS, 128))
    count = lax.axis_size(LAT)
    group = slots.shape[0]
    left = jnp.logical_and(spot < EDGE, lax.rem(spot, 2 * WIDTH) < WIDTH)
    left = jnp.logical_or(left, jnp.logical_and(spot >= EDGE, spot < EDGE + 6))
    tiles = EDGE_COLS // 128
    zero = jnp.zeros((ROWS, 128), jnp.float32)
    fields = [[[zero for _ in range(tiles)] for _ in range(2)] for _ in range(6)]
    for b in range(group // count * (count - 1)):
        slot = b // (count - 1) * count + b % (count - 1)
        pair = jnp.where(left, slots[slot], slots[slot + 1])
        far = turn(pair, -6)
        wets = pair * far
        face = wets * 0.5 * turn(pair + far, -2)
        flux = wets * turn(pair, -4)
        at, home = 16 * (b % 8), b // 8
        here = jnp.logical_and(spot >= at, spot < at + 2 * WIDTH)
        seam = spot == at + WIDTH - 1
        for t in range(2):
            for i in range(4):
                moved = turn(pair, at - 2 * WIDTH * (4 * t + i))
                fields[i][t][home] = jnp.where(here, moved, fields[i][t][home])
            for i, value in enumerate((face, flux)):
                moved = turn(value, at + WIDTH - 1 - EDGE - t)
                fields[4 + i][t][home] = jnp.where(seam, moved, fields[4 + i][t][home])
    fields = [jnp.concatenate([jnp.concatenate(f[t], axis=1) for t in range(2)], axis=0) for f in fields]
    rhs, diag, face_x, face_y, face, flux = fields
    rhs = rhs - flux + pltpu.roll(flux, 1, 1)
    diag = diag + face + pltpu.roll(face, 1, 1)
    face_y = face_y + face
    parts = stencil(face_x, face_y, rhs, diag)
    for i, part in enumerate(parts):
        edge_basis[i] = part
    spot = lane((ROWS, EDGE_COLS))
    column = lax.rem(spot, 16)
    keep = jnp.logical_and(column >= WIDTH - REACH, column < WIDTH + REACH)
    row = add_moments(parts, keep)
    sums = [slots[i] for i in range(group)]
    while len(sums) > 1:
        sums = [sums[i] + sums[i + 1] for i in range(0, len(sums), 2)]
    total = jnp.where(lane((ROWS, 128)) >= MOMENTS, sums[0], pltpu.roll(turn(sums[0], PLAIN - MOMENTS), ROWS - 1, 0))
    moments[...] = jnp.broadcast_to(total[:1] + row, moments.shape)


def poly(a, b, scale):
    size = max(len(a), len(b))
    out = []
    for i in range(size):
        if i >= len(b):
            out.append(a[i])
        elif i >= len(a):
            out.append(scale * b[i])
        else:
            out.append(a[i] + scale * b[i])
    return out


def square(a, gram):
    total = None
    for i in range(len(a)):
        for j in range(i, len(a)):
            term = a[i] * a[j] * gram[i, j]
            term = term if i == j else 2.0 * term
            total = term if total is None else total + term
    return total


def final_kernel(parts, basis, edge_basis, surface, residual):
    row = jnp.sum(parts[...], axis=0, keepdims=True)
    spot = lane((1, 128))
    def at(k):
        return jnp.sum(jnp.where(spot == k, row, 0.0), axis=1, keepdims=True)

    g00, g01, g11, g12, g22, g23 = [at(MOMENTS + k) for k in range(6)]
    m1, m2, m3, m4, m5 = [at(PLAIN + k) for k in range(5)]
    rough = g01 > 0.5 * g00
    newton = {(0, 0): g00, (0, 1): g01, (1, 1): g11, (0, 2): g11 - g01, (1, 2): g12, (2, 2): g22}
    plain = {(0, 0): g00, (0, 1): m1, (1, 1): m2, (0, 2): m2, (1, 2): m3, (2, 2): m4}
    gram = {k: jnp.where(rough, plain[k], newton[k]) for k in plain}
    newton = {(0, 0): g01, (0, 1): g11, (1, 1): g12 + g11, (0, 2): g12, (1, 2): g22 + g12, (2, 2): g23 + g22}
    plain = {(0, 0): g00 - m1, (0, 1): m1 - m2, (1, 1): m2 - m3, (0, 2): m2 - m3, (1, 2): m3 - m4, (2, 2): m4 - m5}
    energy = {k: jnp.where(rough, plain[k], newton[k]) for k in plain}
    stay, shift = jnp.where(rough, 1.0, 0.0), jnp.where(rough, -1.0, 1.0)
    one = jnp.ones((1, 1), jnp.float32)
    pre, direction = [one], [one]
    gamma = g00
    step = gamma / energy[0, 0]
    answer = [step]
    for sweep in range(3):
        image = [stay * direction[0]]
        for i in range(1, sweep + 1):
            image.append(direction[i] + shift * direction[i - 1])
        image.append(shift * direction[-1])
        pre = poly(pre, image, -step)
        if sweep == 2:
            break
        gamma_next = square(pre, gram)
        delta = square(pre, energy)
        ratio = gamma_next / gamma
        step = gamma_next / (delta - ratio * gamma_next / step)
        direction = poly(pre, direction, ratio)
        answer = poly(answer, direction, step)
        gamma = gamma_next
    for coefs in (answer, pre):
        for i in range(len(coefs) - 1, 0, -1):
            coefs[i - 1] = coefs[i - 1] + jnp.where(rough, coefs[i], 0.0)
        for i in range(1, len(coefs), 2):
            coefs[i] = shift * coefs[i]

    def combine(b):
        eta = answer[0] * b[0] + answer[1] * b[1] + answer[2] * b[2]
        return eta, (pre[0] * b[3] + pre[1] * b[4]) + (pre[2] * b[5] + pre[3] * b[6])

    inner, edge = combine(basis), combine(edge_basis)
    place, count = lat_index(), lax.axis_size(LAT)
    group = lax.axis_index("lon_2") * (count - 1)
    spot = lane((ROWS, 128))
    for out, body, strip in ((surface, inner[0], edge[0]), (residual, inner[1], edge[1])):
        out[:, 128 : COLS - 128] = body[:, 128 : COLS - 128]
        for side, ok, base, near in ((-1, place > 0, 0, spot < REACH), (0, place < count - 1, COLS - 128, spot >= 128 - REACH)):
            b = group + place + side
            tile = strip[:, :128]
            for i in range(1, EDGE_COLS // 128):
                tile = pick(b // 8 == i, strip[:, 128 * i : 128 * (i + 1)], tile)
            start = 16 * lax.rem(b, 8) + WIDTH
            moved = pltpu.roll(tile, lax.rem(256 - start, 128), 1)
            use = jnp.logical_and(near, ok)
            out[:, base : base + 128] = jnp.where(use, moved, body[:, base : base + 128])


def kept(*dims):
    return pltpu.VMEM(dims, jnp.float32)


def shape(*dims):
    return jax.ShapeDtypeStruct(dims, jnp.float32)


def call(kernel, name, outs, *args):
    args = [pltpu.with_memory_space_constraint(a, pltpu.VMEM) for a in args]
    specs = jax.tree.map(lambda _: VMEM, outs)
    return pl.pallas_call(kernel, out_shape=outs, in_specs=[VMEM] * len(args), out_specs=specs, name=name)(*args)


def body(u_vel, v_vel, thickness, depth, sea_mask, damping, eta_prev):
    count = lax.axis_size(LON)
    pairs_even = [(i, i ^ 1) for i in range(count)]
    pairs_odd = [(i, (i + 1) % count) if i % 2 else (i, (i - 1) % count) for i in range(count)]
    own, odd, even = pl.pallas_call(
        sum_kernel,
        out_shape=(kept(FIELDS, ROWS, COLS), kept(3, ROWS, COLS), kept(3, ROWS, COLS)),
        in_specs=[ANY] * 7,
        out_specs=(VMEM, VMEM, VMEM),
        scratch_shapes=[
            pltpu.VMEM((LEVELS, ROWS, COLS), jnp.float32),
            pltpu.VMEM((LEVELS, ROWS, COLS), jnp.float32),
            pltpu.VMEM((3, ROWS, COLS), jnp.float32),
            pltpu.VMEM((ROWS, COLS), jnp.int32),
            pltpu.SMEM((LEVELS,), jnp.float32),
            pltpu.SemaphoreType.DMA((2, CHUNKS)),
            pltpu.SemaphoreType.DMA((5,)),
        ],
        name="sums",
    )(thickness, u_vel, v_vel, depth, sea_mask, damping, eta_prev)
    got_odd = lax.ppermute(odd, LON, pairs_odd)
    got_even = lax.ppermute(even, LON, pairs_even)
    near, far = lax.axis_size(NEAR), lax.axis_size(FAR)
    basis, slots = call(block_kernel, "block", (kept(7, ROWS, COLS), kept(near, ROWS, 128)), own, got_odd, got_even)
    slots = lax.all_to_all(slots, NEAR, 0, 0, tiled=True)
    edge_basis, moments = call(edge_kernel, "edge", (kept(7, ROWS, EDGE_COLS), kept(far, 128)), slots)
    moments = lax.all_to_all(moments, FAR, 0, 0, tiled=True)
    outs = (shape(ROWS, COLS), shape(ROWS, COLS))
    return call(final_kernel, "final", outs, moments, basis, edge_basis)


def solution(mesh):
    torus = Mesh(mesh.devices.reshape(8, 8, 4, 2, 2), LON + LAT)
    wide = P(None, LON, LAT)
    flat = P(LON, LAT)
    return jax.shard_map(
        body,
        mesh=torus,
        in_specs=(wide, wide, P(), flat, flat, flat, flat),
        out_specs=(flat, flat),
        check_vma=False,
    )
```
